128 devices in a mesh: shard: 128 (over z, x, y, core).
Axes of the slice: x: 4, y: 4, z: 4, core: 2. Of those that a mesh axis runs over, the one named last changes fastest.
Arguments:
- data_t: bfloat16 [8192, 32768], P('shard'), may hold values from -0.25 to 0.25
- labels: int32 [32768], replicated, may hold values from -1 to 1, as said below
- sample_weight: float32 [32768], replicated, may hold values from 0.1 to 4
- w_start: float32 [8192], P('shard'), may hold values from -10 to 10
- alpha_start: float32 [32768], P('shard'), may hold values from 0 to 1
- visit_order: int32 [256, 128], P('shard'), may hold values from 0 to 127, each once within a row
Outputs:
- weights_out: float32 [8192], P('shard')
- alpha_final: float32 [32768], P('shard')
- objective: float32 [], replicated
The draws below stay inside these ranges and needn't reach their ends.
Inputs may be any that keep to these rules, and one draw needn't show every extreme that they name: `labels`: each label is -1 or +1. `visit_order`: each row is a permutation of 0 to 127.
All inputs are finite; a program needn't handle non-finite values.
Results may differ from the reference program's by a relative error of at most 0.0047.
Values may be sent and summed in bfloat16 or wider, within the bound.
A program may use at most 64 MiB of HBM per device.

```python
import jax
import jax.numpy as jnp
from jax import lax

FEATURES = 8192
BLOCK = 128
GROUP = 16
SAMPLES = 32768
BLOCKS = 256
N_SHARD = 128


def draw_labels(key, part):
    return (2 * jax.random.randint(key, (SAMPLES,), 0, 2) - 1).astype(jnp.int32)


def draw_sample_weight(key, part):
    position = jnp.arange(SAMPLES, dtype=jnp.float32) / (SAMPLES - 1)
    roughness = jnp.exp(jax.random.uniform(key, (SAMPLES,), jnp.float32, -0.35, 0.35))
    return (0.5 * jnp.power(3.0, position) * roughness).astype(jnp.float32)


def draw_w_start(key, part):
    position = jnp.arange(FEATURES, dtype=jnp.float32) / (FEATURES - 1)
    normal_draw = jnp.clip(jax.random.normal(key, (FEATURES,), jnp.float32), -4.0, 4.0)
    return (0.6 * jnp.power(3.0, position) * normal_draw).astype(jnp.float32)


def with_spikes(array, stream_key, source, target, parts, factor):
    owner, partner = [(jnp.arange(array.shape[axis_at]) // (array.shape[axis_at] // parts)).reshape([-1 if axis == axis_at else 1 for axis in range(array.ndim)]) for axis_at in (source, target)]
    chosen = jax.random.permutation(stream_key, parts)[partner]
    strong = (owner == chosen) | (owner == (partner + parts // 2) % parts)
    return jnp.where(strong, factor * array, array)


def steps_of(stream_key, dims, cuts, smallest, high):
    factor_of, own = 1.0, jax.random.fold_in(stream_key, 6)
    for dim, shards_of in cuts:
        heights = jnp.exp(jax.random.uniform(jax.random.fold_in(own, dim), (shards_of,), jnp.float32, smallest / len(cuts), high / len(cuts)))
        factor_of = factor_of * jnp.repeat(heights, dims[dim] // shards_of).reshape([-1 if axis == dim else 1 for axis in range(len(dims))])
    return factor_of


def noise_with(own_key, shape, spread, limit, cuts, heavy, held_as=jnp.bfloat16):
    array = spread * jax.random.normal(own_key, shape, jnp.float32)
    if cuts:
        array = array * steps_of(own_key, shape, cuts, -0.22, 0.18)
    return jnp.clip(with_spikes(array, jax.random.fold_in(own_key, 3), *heavy), -limit, limit).astype(held_as)


def setup_inputs(seed: int = 0) -> dict:
    key_of = jax.random.split(jax.random.key(seed), 7)
    return {
        "data_t": noise_with(key_of[0], (FEATURES, SAMPLES), FEATURES ** -0.5, 0.25, ((0, 128),), (1, 0, 128, 5.5)),
        "labels": draw_labels(jax.random.fold_in(key_of[6], 71), 0),
        "sample_weight": draw_sample_weight(jax.random.fold_in(key_of[6], 71), 0),
        "w_start": draw_w_start(jax.random.fold_in(key_of[6], 71), 0),
        "alpha_start": jnp.clip(1.0 * jax.random.uniform(key_of[4], (SAMPLES,), jnp.float32) ** steps_of(key_of[4], (SAMPLES,), ((0, 128),), -0.2, 0.2), 0.0, 1.0),
        "visit_order": jax.vmap(lambda own: jax.random.permutation(own, BLOCK))(jax.random.split(key_of[5], BLOCKS)).reshape((BLOCKS, BLOCK)).astype(jnp.int32),
    }


def sweep_rows(gram_block, label_rows, bound_rows, alpha_rows, margin_rows, visit_rows):
    gram_perm = gram_block[visit_rows][:, visit_rows]
    label_perm = label_rows[visit_rows]
    bound_perm = bound_rows[visit_rows]
    alpha_perm = alpha_rows[visit_rows]
    margin_perm = margin_rows[visit_rows]
    diag_perm = jnp.diagonal(gram_perm) + 1e-6

    def update_group(group_index, state_pair):
        alpha_now, margin_now = state_pair
        first_row = jnp.asarray(group_index * GROUP).astype(jnp.int32)
        group_alpha = lax.dynamic_slice_in_dim(alpha_now, first_row, GROUP)
        group_label = lax.dynamic_slice_in_dim(label_perm, first_row, GROUP)
        group_margin = lax.dynamic_slice_in_dim(margin_now, first_row, GROUP)
        group_diag = lax.dynamic_slice_in_dim(diag_perm, first_row, GROUP)
        group_bound = lax.dynamic_slice_in_dim(bound_perm, first_row, GROUP)
        fresh_alpha = jnp.clip(group_alpha + (1.0 - group_label * group_margin) / (2.0 * group_diag), 0.0, group_bound)
        change = fresh_alpha - group_alpha
        columns = lax.dynamic_slice_in_dim(gram_perm, first_row, GROUP, 1)
        margin_now = margin_now + 2.0 * jnp.dot(columns, group_label * change, precision=lax.Precision.HIGHEST)
        alpha_now = lax.dynamic_update_slice_in_dim(alpha_now, fresh_alpha, first_row, 0)
        return alpha_now, margin_now

    alpha_perm, margin_perm = lax.fori_loop(0, alpha_rows.shape[0] // GROUP, update_group, (alpha_perm, margin_perm))
    return jnp.zeros_like(alpha_rows).at[visit_rows].set(alpha_perm)


def reference(data_t, labels, sample_weight, w_start, alpha_start, visit_order):
    features, samples = data_t.shape
    devices = N_SHARD
    row_count = samples // devices
    label_sign = labels.astype(jnp.float32)
    start_margin = jnp.dot(w_start.astype(jnp.bfloat16), data_t, preferred_element_type=jnp.float32)
    weighted = (sample_weight * label_sign * jnp.maximum(0.0, 1.0 - label_sign * start_margin)).astype(jnp.bfloat16)
    ascent = jnp.dot(data_t, weighted, preferred_element_type=jnp.float32)
    column_sq = jnp.einsum("fs,fs->f", data_t, data_t, preferred_element_type=jnp.float32)
    scale_col = column_sq / samples + 1e-6
    stepped = w_start + ascent / (samples * scale_col)
    thresh = 1.0 / (4.0 * features * scale_col)
    primal = stepped - jnp.clip(stepped, -thresh, thresh)
    model_margin = jnp.dot(primal.astype(jnp.bfloat16), data_t, preferred_element_type=jnp.float32)
    objective = jnp.sum(sample_weight * jnp.square(jnp.maximum(0.0, 1.0 - label_sign * model_margin))) / (2.0 * samples) + jnp.sum(jnp.abs(primal)) / (4.0 * features)
    block_count = row_count // BLOCK
    visit_rows = visit_order.reshape(devices, block_count, BLOCK) + (jnp.arange(block_count, dtype=jnp.int32) * BLOCK)[None, :, None]
    visit_rows = visit_rows.reshape(devices, row_count).astype(jnp.int32)

    def gram_one(device_number):
        first = (device_number * row_count).astype(jnp.int32)
        piece = lax.dynamic_slice_in_dim(data_t, first, row_count, 1)
        return lax.dot_general(piece, piece, (((0,), (0,)), ((), ())), preferred_element_type=jnp.float32)

    gram_all = lax.map(gram_one, jnp.arange(devices, dtype=jnp.int32))
    sign_dev = label_sign.reshape(devices, row_count)
    bound_dev = sample_weight.reshape(devices, row_count)
    alpha_zero = bound_dev * alpha_start.reshape(devices, row_count)
    sweep_all = jax.vmap(sweep_rows)
    alpha_one = sweep_all(gram_all, sign_dev, bound_dev, alpha_zero, model_margin.reshape(devices, row_count), visit_rows)
    change_one = (sign_dev * (alpha_one - alpha_zero)).reshape(samples).astype(jnp.bfloat16)
    update_one = jnp.dot(data_t, change_one, preferred_element_type=jnp.float32) * (2.0 / devices)
    second_margin = model_margin + jnp.dot(update_one.astype(jnp.bfloat16), data_t, preferred_element_type=jnp.float32)
    alpha_two = sweep_all(gram_all, sign_dev, bound_dev, alpha_one, second_margin.reshape(devices, row_count), visit_rows)
    change_two = (sign_dev * (alpha_two - alpha_one)).reshape(samples).astype(jnp.bfloat16)
    update_two = jnp.dot(data_t, change_two, preferred_element_type=jnp.float32) * (2.0 / devices)
    weights_out = primal + update_one + update_two
    return weights_out, alpha_two.reshape(samples), objective
```

```python
import functools

import jax
import jax.numpy as jnp
from jax import lax
from jax.experimental import pallas as pl
from jax.experimental.pallas import tpu as pltpu
from jax.sharding import PartitionSpec as P

F32 = jnp.float32
BF16 = jnp.bfloat16
MESH = pl.DeviceIdType.MESH
AXIS = "shard"
GROUP = 16
BATCHES = 4


def kernel(devices, samples, x_hbm, lab_hbm, wgt_hbm, w_ref, start_ref, visit_ref,
           weights_ref, alpha_ref, objective_ref,
           x, raw, own_lab, own_wgt, send, recv, h_all, z_all, obj_all,
           gram, perm, onehot, onehot_t, mc, yc, cc, ac, ic, zc, zown,
           load_sem, small_sem, own_sem, bulk_send, bulk_recv,
           rs_send, rs_recv, ag_send, ag_recv, obj_send, obj_recv):
    me = lax.axis_index(AXIS)
    local = x.shape[0]
    features = local * devices
    rows = 256
    others = devices - 1

    def target(k):
        o = lax.rem(k * 37, devices)
        c = lax.rem(me + o, 2)
        y = lax.rem(me // 2 + o // 2, 4)
        xx = lax.rem(me // 8 + o // 8, 4)
        z = lax.rem(me // 32 + o // 32, 4)
        return ((z * 4 + xx) * 4 + y) * 2 + c

    barrier = pltpu.get_barrier_semaphore()

    def greet(k, carry):
        pl.semaphore_signal(barrier, inc=1, device_id=(target(k),), device_id_type=MESH)
        return carry

    lax.fori_loop(1, devices, greet, 0)

    pieces = load_sem.shape[0]
    width = samples // pieces

    def load(i):
        at = pl.ds(i * width, width)
        return pltpu.make_async_copy(x_hbm.at[:, at], x.at[:, at], load_sem.at[i])

    for i in range(pieces):
        load(i).start()
    lab_copy = pltpu.make_async_copy(lab_hbm.at[me], own_lab, small_sem.at[0])
    wgt_copy = pltpu.make_async_copy(wgt_hbm.at[me], own_wgt, small_sem.at[1])
    lab_copy.start()
    wgt_copy.start()
    own_copy = pltpu.make_async_copy(
        x_hbm.at[:, pl.ds(pl.multiple_of(me * rows, rows), rows)], raw.at[others], own_sem
    )
    own_copy.start()

    eye = lax.broadcasted_iota(jnp.int32, (local, local), 0) == lax.broadcasted_iota(
        jnp.int32, (local, local), 1
    )

    def to_row(col):
        return jnp.sum(jnp.where(eye, col, 0.0), axis=0, keepdims=True)

    def to_col(row):
        return jnp.sum(jnp.where(eye, row, 0.0), axis=1, keepdims=True)

    chunk = 2048

    def margins(row, phase, first, last):
        lhs = jnp.broadcast_to(row, (8, local)).astype(BF16)

        def one(i, carry):
            out = jnp.dot(
                lhs, x[:, pl.ds(pl.multiple_of(i * chunk, chunk), chunk)],
                preferred_element_type=F32,
            )
            for j in range(chunk // 128):
                send[phase, i * (chunk // rows) + j // 2, j % 2 : j % 2 + 1, :] = out[
                    0:1, 128 * j : 128 * j + 128
                ]
            return carry

        lax.fori_loop(first, last, one, 0)

    def scatter(phase):
        def one(k, carry):
            to = target(k)
            pltpu.make_async_remote_copy(
                src_ref=send.at[phase, to], dst_ref=recv.at[phase, me],
                send_sem=rs_send.at[phase], recv_sem=rs_recv.at[phase],
                device_id=(to,), device_id_type=MESH,
            ).start()
            return carry

        recv[phase, me] = send[phase, me]
        lax.fori_loop(1, devices, one, 0)

    def scattered(phase):
        many = recv.at[phase, pl.ds(0, others)]
        pltpu.make_async_copy(many, many, rs_recv.at[phase]).wait()
        return jnp.sum(recv[phase], axis=0)

    def gather(src, buf, send_sem, recv_sem):
        def one(k, carry):
            pltpu.make_async_remote_copy(
                src_ref=src, dst_ref=buf.at[me],
                send_sem=send_sem, recv_sem=recv_sem,
                device_id=(target(k),), device_id_type=MESH,
            ).start()
            return carry

        lax.fori_loop(1, devices, one, 0)

    def drain(buf, sem):
        many = buf.at[pl.ds(0, others)]
        pltpu.make_async_copy(many, many, sem).wait()

    def bulk(batch):
        def one(k, carry):
            to = target(k)
            pltpu.make_async_remote_copy(
                src_ref=x.at[:, pl.ds(pl.multiple_of(to * rows, rows), rows)],
                dst_ref=raw.at[k - 1],
                send_sem=bulk_send.at[batch], recv_sem=bulk_recv.at[batch],
                device_id=(to,), device_id_type=MESH,
            ).start()
            return carry

        size = devices // BATCHES
        lax.fori_loop(batch * size + 1, min((batch + 1) * size, others) + 1, one, 0)

    def batch_slots(batch):
        size = devices // BATCHES
        return raw.at[pl.ds(batch * size, min((batch + 1) * size, others) - batch * size)]

    def contract(buf):
        def one(d, acc):
            part = x[:, pl.ds(pl.multiple_of(d * rows, rows), rows)].astype(F32)
            v = buf[d].astype(F32)
            return acc + part[:, :128] * v[0:1] + part[:, 128:] * v[1:2]

        acc = lax.fori_loop(0, devices, one, jnp.zeros((local, 128), F32), unroll=4)
        return jnp.sum(acc, axis=1, keepdims=True)

    w_row = w_ref[...]
    per = width // chunk
    for i in range(pieces):
        load(i).wait()
        margins(w_row, 0, i * per, (i + 1) * per)
    pl.semaphore_wait(barrier, others)
    scatter(0)
    bulk(0)

    def square(d, acc):
        part = x[:, pl.ds(pl.multiple_of(d * rows, rows), rows)].astype(F32)
        return acc + part[:, :128] * part[:, :128] + part[:, 128:] * part[:, 128:]

    sq = lax.fori_loop(0, devices, square, jnp.zeros((local, 128), F32), unroll=4)
    scale = jnp.sum(sq, axis=1, keepdims=True) / samples + 1e-06
    lab_copy.wait()
    wgt_copy.wait()
    sign = own_lab[...].astype(F32)
    bound = own_wgt[...]

    v0 = scattered(0)
    h_all[me] = (bound * sign * jnp.maximum(0.0, 1.0 - sign * v0)).astype(BF16)
    gather(h_all.at[me], h_all, ag_send.at[0], ag_recv.at[0])
    bulk(1)
    alpha0 = bound * start_ref[...]
    lane = lax.broadcasted_iota(jnp.int32, (128, 128), 1)
    sub = lax.broadcasted_iota(jnp.int32, (128, 128), 0)

    def permuted(vec, b):
        col = jnp.sum(onehot[b] * vec[b : b + 1], axis=1, keepdims=True)
        return jnp.broadcast_to(col, (128, 128))

    for b in range(2):
        hot = jnp.where(sub == visit_ref[b : b + 1, :], 1.0, 0.0)
        onehot_t[b] = hot.astype(BF16)
        onehot[b] = jnp.transpose(hot)
    for b in range(2):
        part = slice(128 * b, 128 * b + 128)
        yc[part] = permuted(sign, b)
        cc[part] = permuted(bound, b)
        ac[part] = permuted(alpha0, b)

    drain(h_all, ag_recv.at[0])
    w_col = to_col(w_row)
    stepped = w_col + contract(h_all) / (samples * scale)
    thresh = 1.0 / (4.0 * features * scale)
    primal = stepped - jnp.clip(stepped, -thresh, thresh)
    penalty = jnp.sum(jnp.abs(primal)) / (4.0 * features)
    margins(to_row(primal), 1, 0, samples // chunk)
    scatter(1)
    for batch in range(2, BATCHES):
        bulk(batch)
    v1 = scattered(1)
    loss = jnp.sum(bound * jnp.square(jnp.maximum(0.0, 1.0 - sign * v1))) / (2.0 * samples)
    obj_all[me] = jnp.full((1, 128), loss + penalty, F32)

    own_copy.wait()
    gram[...] = jnp.zeros_like(gram)
    size = devices // BATCHES
    for batch in range(BATCHES):
        slots = batch_slots(batch)
        pltpu.make_async_copy(slots, slots, bulk_recv.at[batch]).wait()

        def one(i, carry):
            piece = raw[pl.ds(batch * size + i * 16, 16)].reshape(16 * local, rows)
            gram[...] += lax.dot_general(
                piece, piece, (((0,), (0,)), ((), ())), preferred_element_type=F32
            )
            return carry

        lax.fori_loop(0, size // 16, one, 0)

    def halves(a):
        hi = a.astype(BF16)
        return hi, (a - hi.astype(F32)).astype(BF16)

    for b in range(2):
        cols = slice(128 * b, 128 * b + 128)
        hi, lo = halves(gram[:, cols])
        perm[:, cols] = jnp.dot(hi, onehot_t[b], preferred_element_type=F32) + jnp.dot(
            lo, onehot_t[b], preferred_element_type=F32
        )
    for b in range(2):
        part = slice(128 * b, 128 * b + 128)
        left = onehot[b].astype(BF16)
        hi, lo = halves(perm[part, :])
        gram[part, :] = jnp.dot(left, hi, preferred_element_type=F32) + jnp.dot(
            left, lo, preferred_element_type=F32
        )
    for b in range(2):
        part = slice(128 * b, 128 * b + 128)
        diag = jnp.sum(jnp.where(lane == sub, gram[part, part], 0.0), axis=1, keepdims=True)
        ic[part] = jnp.broadcast_to(1.0 / (2.0 * (diag + 1e-06)), (128, 128))

    lane16 = lax.broadcasted_iota(jnp.int32, (GROUP, 128), 1)
    sub16 = lax.broadcasted_iota(jnp.int32, (GROUP, 128), 0)

    def sweep(margin):
        for b in range(2):
            mc[128 * b : 128 * b + 128] = permuted(margin, b)
        c = [jnp.zeros((1, 128), F32), jnp.zeros((1, 128), F32)]
        for t in range(rows // GROUP):
            at = slice(GROUP * t, GROUP * t + GROUP)
            b, first = t // 8, GROUP * (t % 8)
            prod = gram[at, 0:128] * c[0]
            if b:
                prod = prod + gram[at, 128:256] * c[1]
            m = mc[at] + 2.0 * jnp.sum(prod, axis=1, keepdims=True)
            old, y = ac[at], yc[at]
            new = jnp.clip(old + (1.0 - y * m) * ic[at], 0.0, cc[at])
            step = y * (new - old)
            ac[at] = new
            zc[at] = step
            c[b] = c[b] + jnp.sum(
                jnp.where(lane16 == sub16 + first, step, 0.0), axis=0, keepdims=True
            )

    def natural(col, b):
        return jnp.sum(onehot[b] * col[128 * b : 128 * b + 128], axis=0, keepdims=True)

    sweep(v1)
    for b in range(2):
        zown[b : b + 1] = natural(zc, b)
    z_all[0, me] = zown[...].astype(BF16)
    gather(z_all.at[0, me], z_all.at[0], ag_send.at[1], ag_recv.at[1])
    gather(obj_all.at[me], obj_all, obj_send, obj_recv)
    drain(z_all.at[0], ag_recv.at[1])
    first_dw = contract(z_all.at[0]) * (2.0 / devices)
    margins(to_row(first_dw), 2, 0, samples // chunk)
    scatter(2)
    v2 = v1 + scattered(2)
    sweep(v2)
    for b in range(2):
        zown[b : b + 1] = natural(zc, b)
    z_all[1, me] = zown[...].astype(BF16)
    gather(z_all.at[1, me], z_all.at[1], ag_send.at[2], ag_recv.at[2])
    for b in range(2):
        alpha_ref[b : b + 1] = natural(ac, b)
    drain(obj_all, obj_recv)
    objective_ref[...] = jnp.sum(obj_all[...], axis=0)
    for phase in range(3):
        drain(send.at[phase], rs_send.at[phase])
    drain(h_all, ag_send.at[0])
    drain(z_all.at[0], ag_send.at[1])
    drain(obj_all, obj_send)
    for batch in range(BATCHES):
        slots = batch_slots(batch)
        pltpu.make_async_copy(slots, slots, bulk_send.at[batch]).wait()
    drain(z_all.at[1], ag_recv.at[2])
    second_dw = contract(z_all.at[1]) * (2.0 / devices)
    weights_ref[...] = to_row(primal + first_dw + second_dw)
    drain(z_all.at[1], ag_send.at[2])


def solution(mesh):
    devices = mesh.shape[AXIS]

    def body(data_t, labels, sample_weight, w_start, alpha_start, visit_order):
        local, samples = data_t.shape
        per = samples // devices
        anyspace = pl.BlockSpec(memory_space=pl.ANY)
        vmem = pl.BlockSpec(memory_space=pltpu.VMEM)
        square = pltpu.VMEM((per, 128), F32)
        dma = pltpu.SemaphoreType.DMA
        weights, alpha, objective = pl.pallas_call(
            functools.partial(kernel, devices, samples),
            out_shape=(
                jax.ShapeDtypeStruct((1, local), F32),
                jax.ShapeDtypeStruct((2, 128), F32),
                jax.ShapeDtypeStruct((1, 128), F32),
            ),
            in_specs=[anyspace, anyspace, anyspace, vmem, vmem, vmem],
            out_specs=(vmem, vmem, vmem),
            scratch_shapes=[
                pltpu.VMEM((local, samples), BF16),
                pltpu.VMEM((devices, local, per), BF16),
                pltpu.VMEM((2, 128), jnp.int32),
                pltpu.VMEM((2, 128), F32),
                pltpu.VMEM((3, devices, 2, 128), F32),
                pltpu.VMEM((3, devices, 2, 128), F32),
                pltpu.VMEM((devices, 2, 128), BF16),
                pltpu.VMEM((2, devices, 2, 128), BF16),
                pltpu.VMEM((devices, 1, 128), F32),
                pltpu.VMEM((per, per), F32),
                pltpu.VMEM((per, per), F32),
                pltpu.VMEM((2, 128, 128), F32),
                pltpu.VMEM((2, 128, 128), BF16),
                square, square, square, square, square, square,
                pltpu.VMEM((2, 128), F32),
                dma((8,)), dma((2,)), dma, dma((BATCHES,)), dma((BATCHES,)),
                dma((3,)), dma((3,)), dma((3,)), dma((3,)), dma, dma,
            ],
            compiler_params=pltpu.CompilerParams(collective_id=0, has_side_effects=True),
        )(
            data_t,
            labels.reshape(devices, 2, 128),
            sample_weight.reshape(devices, 2, 128),
            w_start.reshape(1, local),
            alpha_start.reshape(2, 128),
            visit_order,
        )
        return weights.reshape(local), alpha.reshape(per), objective[0, 0]

    return jax.shard_map(
        body,
        mesh=mesh,
        in_specs=(P(AXIS, None), P(), P(), P(AXIS), P(AXIS), P(AXIS, None)),
        out_specs=(P(AXIS), P(AXIS), P()),
        check_vma=False,
    )
```

```python
import functools

import jax
import jax.numpy as jnp
from jax import lax
from jax.experimental import pallas as pl
from jax.experimental.pallas import tpu as pltpu
from jax.sharding import PartitionSpec as P

F32 = jnp.float32
BF16 = jnp.bfloat16
MESH = pl.DeviceIdType.MESH
AXIS = "shard"
GROUP = 16
ORDER = (2, 1, 3, 0)


def kernel(devices, samples, x_hbm, lab_hbm, wgt_hbm, w_hbm, start_hbm, visit_hbm,
           weights_ref, alpha_ref, objective_ref,
           x, raw, pout, part_all, own_lab, own_wgt, w_ref, start_ref, visit_ref,
           send, recv, h_all, z_all, obj_all,
           gram, onehot, onehot_t, mc, yc, cc, ac, ic, zc, zown,
           load_sem, small_sem, own_sem, bulk_send, bulk_recv, part_send, part_recv,
           rs_send, rs_recv, ag_send, ag_recv, obj_send, obj_recv):
    me = lax.axis_index(AXIS)
    local = x.shape[0]
    features = local * devices
    rows = 256
    others = devices - 1

    my_z, my_x, my_y, my_c = me // 32, lax.rem(me // 8, 4), lax.rem(me // 2, 4), lax.rem(me, 2)
    near = [lax.rem(my_y + j // 2, 4) * 2 + lax.rem(my_c + j % 2, 2) for j in range(8)]

    def peers(first, last, visit):
        def one(i, carry):
            base = lax.rem(my_z + i // 4, 4) * 32 + lax.rem(my_x + lax.rem(i, 4), 4) * 8
            for j in range(8):
                visit(base + near[j], i * 8 + j)
            return carry

        if first == 0:
            for j in range(1, 8):
                visit(my_z * 32 + my_x * 8 + near[j], j)
        lax.fori_loop(max(first, 1), last, one, 0)

    barrier = pltpu.get_barrier_semaphore()

    def greet(to, k):
        pl.semaphore_signal(barrier, inc=1, device_id=(to,), device_id_type=MESH)

    peers(0, 16, greet)

    pieces = load_sem.shape[0]
    width = samples // pieces

    def load(i):
        at = pl.ds(i * width, width)
        return pltpu.make_async_copy(x_hbm.at[:, at], x.at[:, at], load_sem.at[i])

    small = [
        pltpu.make_async_copy(src, dst, small_sem.at[i])
        for i, (src, dst) in enumerate(
            (
                (w_hbm, w_ref),
                (lab_hbm.at[me], own_lab),
                (wgt_hbm.at[me], own_wgt),
                (start_hbm, start_ref),
                (visit_hbm, visit_ref),
            )
        )
    ]
    small[0].start()
    for i in range(pieces):
        load(i).start()
    for copy in small[1:]:
        copy.start()

    def slice_of(to):
        return pl.ds(pl.multiple_of(to * rows, rows), rows)

    def group_of(line, b, yy, place, core):
        if line == 0:
            return ((place * 4 + lax.rem(my_x + ORDER[b], 4)) * 4 + yy) * 2 + core
        return ((lax.rem(my_z + ORDER[b], 4) * 4 + place) * 4 + 2 + yy) * 2 + core

    def collector(line, place, core):
        if line == 0:
            return ((place * 4 + my_x) * 4 + my_y) * 2 + core
        return ((my_z * 4 + place) * 4 + my_y) * 2 + core

    my_place = (my_z, my_x)

    def own_slices(b):
        return [
            pltpu.make_async_copy(
                x_hbm.at[:, slice_of(group_of(line, b, yy, my_place[line], my_c))],
                raw.at[line, 2 * b + yy, my_place[line] * 2 + my_c],
                own_sem.at[line, 2 * b + yy],
            )
            for yy in range(2)
            for line in range(2)
        ]

    def bulk(b):
        for yy in range(2):
            for step, other in ((1, 0), (3, 0), (2, 1), (0, 1), (1, 1), (3, 1), (2, 0)):
                for line in range(2):
                    place = lax.rem(my_place[line] + step, 4)
                    core = lax.rem(my_c + other, 2)
                    pltpu.make_async_remote_copy(
                        src_ref=x.at[:, slice_of(group_of(line, b, yy, place, core))],
                        dst_ref=raw.at[line, 2 * b + yy, my_place[line] * 2 + my_c],
                        send_sem=bulk_send.at[line, b], recv_sem=bulk_recv.at[line, b],
                        device_id=(collector(line, place, core),), device_id_type=MESH,
                    ).start()

    def bulk_wait(b, sem):
        for line in range(2):
            slots = raw.at[line, pl.ds(2 * b, 2), pl.ds(0, 7)]
            pltpu.make_async_copy(slots, slots, sem.at[line, b]).wait()

    lane = lax.broadcasted_iota(jnp.int32, (128, 128), 1)
    sub = lax.broadcasted_iota(jnp.int32, (128, 128), 0)

    def partial_gram(b):
        for copy in own_slices(b):
            copy.wait()
        bulk_wait(b, bulk_recv)
        for line in range(2):
            for yy in range(2):
                at = line * 8 + 2 * b + yy
                piece = raw[line, 2 * b + yy].reshape(8 * local, rows)
                full = lax.dot_general(
                    piece, piece, (((0,), (0,)), ((), ())), preferred_element_type=F32
                )
                first, last = full[:128, :128], full[128:, 128:]
                pout[at, 0:128] = jnp.where(sub > lane, first, last).astype(BF16)
                pout[at, 128:256] = full[128:, :128].astype(BF16)
                diag = jnp.sum(jnp.where(sub == lane, first, 0.0), axis=0, keepdims=True)
                pout[at, 256:272] = jnp.broadcast_to(diag, (16, 128)).astype(BF16)
                owner = group_of(line, b, yy, my_place[line], my_c)
                slot = (my_x, my_z)[line] * 4 + my_y

                @pl.when(owner == me)
                def _():
                    part_all[slot] = pout[at]

                @pl.when(owner != me)
                def _():
                    pltpu.make_async_remote_copy(
                        src_ref=pout.at[at], dst_ref=part_all.at[slot],
                        send_sem=part_send, recv_sem=part_recv,
                        device_id=(owner,), device_id_type=MESH,
                    ).start()

    def partials(sem):
        many = part_all.at[pl.ds(0, 15)]
        pltpu.make_async_copy(many, many, sem).wait()

    for b in range(4):
        for copy in own_slices(b):
            copy.start()

    eye = lax.broadcasted_iota(jnp.int32, (local, local), 0) == lax.broadcasted_iota(
        jnp.int32, (local, local), 1
    )

    def to_row(col):
        return jnp.sum(jnp.where(eye, col, 0.0), axis=0, keepdims=True)

    def to_col(row):
        return jnp.sum(jnp.where(eye, row, 0.0), axis=1, keepdims=True)

    chunk = samples // 4

    def margins(row, phase, first, last):
        lhs = jnp.broadcast_to(row, (8, local)).astype(BF16)

        def one(i, carry):
            out = jnp.dot(
                lhs, x[:, pl.ds(pl.multiple_of(i * chunk, chunk), chunk)],
                preferred_element_type=F32,
            )
            for j in range(chunk // 128):
                send[phase, i * (chunk // rows) + j // 2, j % 2 : j % 2 + 1, :] = out[
                    0:1, 128 * j : 128 * j + 128
                ]
            return carry

        lax.fori_loop(first, last, one, 0)

    def scatter(phase):
        def one(to, k):
            pltpu.make_async_remote_copy(
                src_ref=send.at[phase, to], dst_ref=recv.at[phase, me],
                send_sem=rs_send.at[phase], recv_sem=rs_recv.at[phase],
                device_id=(to,), device_id_type=MESH,
            ).start()

        recv[phase, me] = send[phase, me]
        peers(0, 16, one)

    def scattered(phase):
        many = recv.at[phase, pl.ds(0, others)]
        pltpu.make_async_copy(many, many, rs_recv.at[phase]).wait()
        return jnp.sum(recv[phase], axis=0)

    def gather(src, buf, send_sem, recv_sem):
        def one(to, k):
            pltpu.make_async_remote_copy(
                src_ref=src, dst_ref=buf.at[me],
                send_sem=send_sem, recv_sem=recv_sem,
                device_id=(to,), device_id_type=MESH,
            ).start()

        peers(0, 16, one)

    def drain(buf, sem):
        many = buf.at[pl.ds(0, others)]
        pltpu.make_async_copy(many, many, sem).wait()

    def contract(buf):
        def one(d, acc):
            part = x[:, pl.ds(pl.multiple_of(d * rows, rows), rows)].astype(F32)
            v = buf[d].astype(F32)
            return acc + part[:, :128] * v[0:1] + part[:, 128:] * v[1:2]

        acc = lax.fori_loop(0, devices, one, jnp.zeros((local, 128), F32), unroll=4)
        return jnp.sum(acc, axis=1, keepdims=True)

    small[0].wait()
    w_row = w_ref[...]
    per = width // chunk
    for i in range(pieces):
        load(i).wait()
        margins(w_row, 0, i * per, (i + 1) * per)
    pl.semaphore_wait(barrier, others)
    scatter(0)
    bulk(0)

    def square(d, acc):
        part = x[:, pl.ds(pl.multiple_of(d * rows, rows), rows)].astype(F32)
        return acc + part[:, :128] * part[:, :128] + part[:, 128:] * part[:, 128:]

    sq = lax.fori_loop(0, devices, square, jnp.zeros((local, 128), F32), unroll=4)
    scale = jnp.sum(sq, axis=1, keepdims=True) / samples + 1e-06
    for copy in small[1:]:
        copy.wait()
    sign = own_lab[...].astype(F32)
    bound = own_wgt[...]

    v0 = scattered(0)
    h_all[me] = (bound * sign * jnp.maximum(0.0, 1.0 - sign * v0)).astype(BF16)
    gather(h_all.at[me], h_all, ag_send.at[0], ag_recv.at[0])
    bulk(1)
    alpha0 = bound * start_ref[...]

    def permuted(vec, b):
        col = jnp.sum(onehot[b] * vec[b : b + 1], axis=1, keepdims=True)
        return jnp.broadcast_to(col, (128, 128))

    for b in range(2):
        hot = jnp.where(sub == visit_ref[b : b + 1, :], 1.0, 0.0)
        onehot_t[b] = hot.astype(BF16)
        onehot[b] = jnp.transpose(hot)
    for b in range(2):
        part = slice(128 * b, 128 * b + 128)
        yc[part] = permuted(sign, b)
        cc[part] = permuted(bound, b)
        ac[part] = permuted(alpha0, b)

    partial_gram(0)
    drain(h_all, ag_recv.at[0])
    w_col = to_col(w_row)
    stepped = w_col + contract(h_all) / (samples * scale)
    thresh = 1.0 / (4.0 * features * scale)
    primal = stepped - jnp.clip(stepped, -thresh, thresh)
    penalty = jnp.sum(jnp.abs(primal)) / (4.0 * features)
    margins(to_row(primal), 1, 0, samples // chunk)
    scatter(1)
    bulk(2)
    bulk(3)
    partial_gram(1)
    v1 = scattered(1)
    loss = jnp.sum(bound * jnp.square(jnp.maximum(0.0, 1.0 - sign * v1))) / (2.0 * samples)
    obj_all[me] = jnp.full((1, 128), loss + penalty, F32)

    partial_gram(2)
    partial_gram(3)
    partials(part_recv)

    def halves(a):
        hi = a.astype(BF16)
        return hi, (a - hi.astype(F32)).astype(BF16)

    def reordered(a, b1, b2):
        hi, lo = halves(a)
        mid = jnp.dot(hi, onehot_t[b2], preferred_element_type=F32) + jnp.dot(
            lo, onehot_t[b2], preferred_element_type=F32
        )
        hi, lo = halves(mid)
        left = onehot[b1].astype(BF16)
        return jnp.dot(left, hi, preferred_element_type=F32) + jnp.dot(
            left, lo, preferred_element_type=F32
        )

    packed = jnp.sum(part_all[:, 0:128].astype(F32), axis=0)
    turned = jnp.transpose(packed)
    diag_row = jnp.sum(part_all[:, 256:272].astype(F32), axis=0)[0:1]
    first_block = jnp.where(sub > lane, packed, jnp.where(sub < lane, turned, diag_row))
    last_block = jnp.where(sub > lane, turned, packed)
    gram[0:128, 0:128] = reordered(first_block, 0, 0)
    gram[128:256, 0:128] = reordered(jnp.sum(part_all[:, 128:256].astype(F32), axis=0), 1, 0)
    gram[128:256, 128:256] = reordered(last_block, 1, 1)
    for b in range(2):
        part = slice(128 * b, 128 * b + 128)
        diag = jnp.sum(jnp.where(lane == sub, gram[part, part], 0.0), axis=1, keepdims=True)
        ic[part] = jnp.broadcast_to(1.0 / (2.0 * (diag + 1e-06)), (128, 128))

    lane16 = lax.broadcasted_iota(jnp.int32, (GROUP, 128), 1)
    sub16 = lax.broadcasted_iota(jnp.int32, (GROUP, 128), 0)

    def sweep(margin):
        for b in range(2):
            mc[128 * b : 128 * b + 128] = permuted(margin, b)
        c = [jnp.zeros((1, 128), F32), jnp.zeros((1, 128), F32)]
        for t in range(rows // GROUP):
            at = slice(GROUP * t, GROUP * t + GROUP)
            b, first = t // 8, GROUP * (t % 8)
            prod = gram[at, 0:128] * c[0]
            if b:
                prod = prod + gram[at, 128:256] * c[1]
            m = mc[at] + 2.0 * jnp.sum(prod, axis=1, keepdims=True)
            old, y = ac[at], yc[at]
            new = jnp.clip(old + (1.0 - y * m) * ic[at], 0.0, cc[at])
            step = y * (new - old)
            ac[at] = new
            zc[at] = step
            c[b] = c[b] + jnp.sum(
                jnp.where(lane16 == sub16 + first, step, 0.0), axis=0, keepdims=True
            )

    def natural(col, b):
        return jnp.sum(onehot[b] * col[128 * b : 128 * b + 128], axis=0, keepdims=True)

    sweep(v1)
    for b in range(2):
        zown[b : b + 1] = natural(zc, b)
    z_all[0, me] = zown[...].astype(BF16)
    gather(z_all.at[0, me], z_all.at[0], ag_send.at[1], ag_recv.at[1])
    gather(obj_all.at[me], obj_all, obj_send, obj_recv)
    drain(z_all.at[0], ag_recv.at[1])
    first_dw = contract(z_all.at[0]) * (2.0 / devices)
    margins(to_row(first_dw), 2, 0, samples // chunk)
    scatter(2)
    v2 = v1 + scattered(2)
    sweep(v2)
    for b in range(2):
        zown[b : b + 1] = natural(zc, b)
    z_all[1, me] = zown[...].astype(BF16)
    gather(z_all.at[1, me], z_all.at[1], ag_send.at[2], ag_recv.at[2])
    for b in range(2):
        alpha_ref[b : b + 1] = natural(ac, b)
    drain(obj_all, obj_recv)
    objective_ref[...] = jnp.sum(obj_all[...], axis=0)
    for phase in range(3):
        drain(send.at[phase], rs_send.at[phase])
    drain(h_all, ag_send.at[0])
    drain(z_all.at[0], ag_send.at[1])
    drain(obj_all, obj_send)
    for b in range(4):
        bulk_wait(b, bulk_send)
    partials(part_send)
    drain(z_all.at[1], ag_recv.at[2])
    second_dw = contract(z_all.at[1]) * (2.0 / devices)
    weights_ref[...] = to_row(primal + first_dw + second_dw)
    drain(z_all.at[1], ag_send.at[2])


def solution(mesh):
    devices = mesh.shape[AXIS]

    def body(data_t, labels, sample_weight, w_start, alpha_start, visit_order):
        local, samples = data_t.shape
        per = samples // devices
        anyspace = pl.BlockSpec(memory_space=pl.ANY)
        vmem = pl.BlockSpec(memory_space=pltpu.VMEM)
        square = pltpu.VMEM((per, 128), F32)
        dma = pltpu.SemaphoreType.DMA
        weights, alpha, objective = pl.pallas_call(
            functools.partial(kernel, devices, samples),
            out_shape=(
                jax.ShapeDtypeStruct((1, local), F32),
                jax.ShapeDtypeStruct((2, 128), F32),
                jax.ShapeDtypeStruct((1, 128), F32),
            ),
            in_specs=[anyspace] * 6,
            out_specs=(vmem, vmem, vmem),
            scratch_shapes=[
                pltpu.VMEM((local, samples), BF16),
                pltpu.VMEM((2, 8, 8, local, per), BF16),
                pltpu.VMEM((16, 272, 128), BF16),
                pltpu.VMEM((16, 272, 128), BF16),
                pltpu.VMEM((2, 128), jnp.int32),
                pltpu.VMEM((2, 128), F32),
                pltpu.VMEM((1, local), F32),
                pltpu.VMEM((2, 128), F32),
                pltpu.VMEM((2, 128), jnp.int32),
                pltpu.VMEM((3, devices, 2, 128), F32),
                pltpu.VMEM((3, devices, 2, 128), F32),
                pltpu.VMEM((devices, 2, 128), BF16),
                pltpu.VMEM((2, devices, 2, 128), BF16),
                pltpu.VMEM((devices, 1, 128), F32),
                pltpu.VMEM((per, per), F32),
                pltpu.VMEM((2, 128, 128), F32),
                pltpu.VMEM((2, 128, 128), BF16),
                square, square, square, square, square, square,
                pltpu.VMEM((2, 128), F32),
                dma((4,)), dma((5,)), dma((2, 8)), dma((2, 4)), dma((2, 4)), dma, dma,
                dma((3,)), dma((3,)), dma((3,)), dma((3,)), dma, dma,
            ],
            compiler_params=pltpu.CompilerParams(collective_id=0, has_side_effects=True),
        )(
            data_t,
            labels.reshape(devices, 2, 128),
            sample_weight.reshape(devices, 2, 128),
            w_start.reshape(1, local),
            alpha_start.reshape(2, 128),
            visit_order,
        )
        return weights.reshape(local), alpha.reshape(per), objective[0, 0]

    return jax.shard_map(
        body,
        mesh=mesh,
        in_specs=(P(AXIS, None), P(), P(), P(AXIS), P(AXIS), P(AXIS, None)),
        out_specs=(P(AXIS), P(AXIS), P()),
        check_vma=False,
    )
```

```python
import functools

import jax
import jax.numpy as jnp
from jax import lax
from jax.experimental import pallas as pl
from jax.experimental.pallas import tpu as pltpu
from jax.sharding import PartitionSpec as P

F32 = jnp.float32
BF16 = jnp.bfloat16
MESH = pl.DeviceIdType.MESH
AXIS = "shard"
GROUP = 16
ORDER = (2, 1, 3, 0)


def kernel(devices, samples, x_hbm, lab_hbm, wgt_hbm, w_hbm, start_hbm, visit_hbm,
           weights_ref, alpha_ref, objective_ref,
           x, raw, pout, mid, psum, fin, own_sum, own_lab, own_wgt, w_ref, start_ref, visit_ref,
           send, recv, h_all, z_all, obj_all,
           gram, onehot, onehot_t, mc, yc, cc, ac, ic, zc, zown,
           load_sem, small_sem, own_sem, bulk_send, bulk_recv, mid_send, mid_recv, fin_send, fin_recv,
           rs_send, rs_recv, ag_send, ag_recv, obj_send, obj_recv):
    me = lax.axis_index(AXIS)
    local = x.shape[0]
    features = local * devices
    rows = 256
    others = devices - 1

    my_z, my_x, my_y, my_c = me // 32, lax.rem(me // 8, 4), lax.rem(me // 2, 4), lax.rem(me, 2)
    near = [
        lax.rem(my_y + dy, 4) * 2 + lax.rem(my_c + dc, 2)
        for dy in (2, 1, 3, 0)
        for dc in (1, 0)
    ]

    def peers(visit):
        def one(i, carry):
            base = (
                lax.rem(my_z + 2 + i // 4, 4) * 32 + lax.rem(my_x + 2 + lax.rem(i, 4), 4) * 8
            )
            for place in near:
                visit(base + place)
            return carry

        lax.fori_loop(0, 10, one, 0)
        lax.fori_loop(11, 16, one, 0)
        for place in near[:7]:
            visit(my_z * 32 + my_x * 8 + place)

    barrier = pltpu.get_barrier_semaphore()

    def greet(to):
        pl.semaphore_signal(barrier, inc=1, device_id=(to,), device_id_type=MESH)

    pieces = load_sem.shape[0]
    width = samples // pieces

    def load(i):
        at = pl.ds(i * width, width)
        return pltpu.make_async_copy(x_hbm.at[:, at], x.at[:, at], load_sem.at[i])

    small = [
        pltpu.make_async_copy(src, dst, small_sem.at[i])
        for i, (src, dst) in enumerate(
            (
                (w_hbm, w_ref),
                (lab_hbm.at[me], own_lab),
                (wgt_hbm.at[me], own_wgt),
                (start_hbm, start_ref),
                (visit_hbm, visit_ref),
            )
        )
    ]
    small[0].start()
    for i in range(pieces):
        load(i).start()
    peers(greet)
    for copy in small[1:]:
        copy.start()

    def slice_of(to):
        return pl.ds(pl.multiple_of(to * rows, rows), rows)

    def group_of(line, b, yy, place, core):
        if line == 0:
            return ((place * 4 + lax.rem(my_x + ORDER[b], 4)) * 4 + yy) * 2 + core
        return ((lax.rem(my_z + ORDER[b], 4) * 4 + place) * 4 + 2 + yy) * 2 + core

    def collector(line, place, core):
        if line == 0:
            return ((place * 4 + my_x) * 4 + my_y) * 2 + core
        return ((my_z * 4 + place) * 4 + my_y) * 2 + core

    my_place = (my_z, my_x)

    def own_slices(b):
        return [
            pltpu.make_async_copy(
                x_hbm.at[:, slice_of(group_of(line, b, yy, my_place[line], my_c))],
                raw.at[line, 2 * b + yy, my_place[line] * 2 + my_c],
                own_sem.at[line, 2 * b + yy],
            )
            for yy in range(2)
            for line in range(2)
        ]

    def bulk(b):
        for yy in range(2):
            for step, other in ((1, 0), (3, 0), (2, 1), (0, 1), (1, 1), (3, 1), (2, 0)):
                for line in range(2):
                    place = lax.rem(my_place[line] + step, 4)
                    core = lax.rem(my_c + other, 2)
                    pltpu.make_async_remote_copy(
                        src_ref=x.at[:, slice_of(group_of(line, b, yy, place, core))],
                        dst_ref=raw.at[line, 2 * b + yy, my_place[line] * 2 + my_c],
                        send_sem=bulk_send.at[line, b], recv_sem=bulk_recv.at[line, b],
                        device_id=(collector(line, place, core),), device_id_type=MESH,
                    ).start()

    def bulk_wait(b, sem):
        for line in range(2):
            slots = raw.at[line, pl.ds(2 * b, 2), pl.ds(0, 7)]
            pltpu.make_async_copy(slots, slots, sem.at[line, b]).wait()

    lane = lax.broadcasted_iota(jnp.int32, (128, 128), 1)
    sub = lax.broadcasted_iota(jnp.int32, (128, 128), 0)

    def to_row_owner(b, dy):
        y = lax.rem(my_y + dy, 4)
        return pltpu.make_async_remote_copy(
            src_ref=pout.at[b, y], dst_ref=mid.at[b, dy - 1],
            send_sem=mid_send.at[b], recv_sem=mid_recv.at[b],
            device_id=((my_z * 4 + my_x) * 8 + y * 2 + my_c,), device_id_type=MESH,
        )

    def partial_gram(b):
        for copy in own_slices(b):
            copy.wait()
        bulk_wait(b, bulk_recv)
        for line in range(2):
            for yy in range(2):
                at = line * 2 + yy
                piece = raw[line, 2 * b + yy].reshape(8 * local, rows)
                full = lax.dot_general(
                    piece, piece, (((0,), (0,)), ((), ())), preferred_element_type=F32
                )
                first, last = full[:128, :128], full[128:, 128:]
                pout[b, at, 0:128] = jnp.where(sub > lane, first, last).astype(BF16)
                pout[b, at, 128:256] = full[128:, :128].astype(BF16)
                diag = jnp.sum(jnp.where(sub == lane, first, 0.0), axis=0, keepdims=True)
                pout[b, at, 256:272] = jnp.broadcast_to(diag, (16, 128)).astype(BF16)
        for dy in (2, 1, 3):
            to_row_owner(b, dy).start()

    def middle(b):
        pltpu.make_async_copy(mid.at[b], mid.at[b], mid_recv.at[b]).wait()
        total = pout[b, my_y].astype(F32) + jnp.sum(mid[b].astype(F32), axis=0)
        if ORDER[b] == 0:
            own_sum[...] = total
        else:
            line = my_y // 2
            z = lax.rem(my_z + ORDER[b] * line, 4)
            xx = lax.rem(my_x + ORDER[b] * (1 - line), 4)
            psum[b] = total.astype(BF16)
            pltpu.make_async_remote_copy(
                src_ref=psum.at[b], dst_ref=fin.at[b], send_sem=fin_send, recv_sem=fin_recv,
                device_id=((z * 4 + xx) * 8 + my_y * 2 + my_c,), device_id_type=MESH,
            ).start()

    for b in range(4):
        for copy in own_slices(b):
            copy.start()

    eye = lax.broadcasted_iota(jnp.int32, (local, local), 0) == lax.broadcasted_iota(
        jnp.int32, (local, local), 1
    )

    def to_row(col):
        return jnp.sum(jnp.where(eye, col, 0.0), axis=0, keepdims=True)

    def to_col(row):
        return jnp.sum(jnp.where(eye, row, 0.0), axis=1, keepdims=True)

    chunk = samples // 4

    def margins(row, phase, first, last):
        lhs = jnp.broadcast_to(row, (8, local)).astype(BF16)

        def one(i, carry):
            out = jnp.dot(
                lhs, x[:, pl.ds(pl.multiple_of(i * chunk, chunk), chunk)],
                preferred_element_type=F32,
            )
            for j in range(chunk // 128):
                send[phase, i * (chunk // rows) + j // 2, j % 2 : j % 2 + 1, :] = out[
                    0:1, 128 * j : 128 * j + 128
                ]
            return carry

        lax.fori_loop(first, last, one, 0)

    def scatter(phase):
        def one(to):
            pltpu.make_async_remote_copy(
                src_ref=send.at[phase, to], dst_ref=recv.at[phase, me],
                send_sem=rs_send.at[phase], recv_sem=rs_recv.at[phase],
                device_id=(to,), device_id_type=MESH,
            ).start()

        recv[phase, me] = send[phase, me]
        peers(one)

    def scattered(phase):
        many = recv.at[phase, pl.ds(0, others)]
        pltpu.make_async_copy(many, many, rs_recv.at[phase]).wait()
        return jnp.sum(recv[phase], axis=0)

    def gather(src, buf, send_sem, recv_sem):
        def one(to):
            pltpu.make_async_remote_copy(
                src_ref=src, dst_ref=buf.at[me],
                send_sem=send_sem, recv_sem=recv_sem,
                device_id=(to,), device_id_type=MESH,
            ).start()

        peers(one)

    def drain(buf, sem):
        many = buf.at[pl.ds(0, others)]
        pltpu.make_async_copy(many, many, sem).wait()

    def contract(buf):
        def one(d, acc):
            part = x[:, pl.ds(pl.multiple_of(d * rows, rows), rows)].astype(F32)
            v = buf[d].astype(F32)
            return acc + part[:, :128] * v[0:1] + part[:, 128:] * v[1:2]

        acc = lax.fori_loop(0, devices, one, jnp.zeros((local, 128), F32), unroll=4)
        return jnp.sum(acc, axis=1, keepdims=True)

    small[0].wait()
    w_row = w_ref[...]
    per = width // chunk
    for i in range(pieces):
        load(i).wait()
        margins(w_row, 0, i * per, (i + 1) * per)
    pl.semaphore_wait(barrier, others)
    scatter(0)
    bulk(0)

    def square(d, acc):
        part = x[:, pl.ds(pl.multiple_of(d * rows, rows), rows)].astype(F32)
        return acc + part[:, :128] * part[:, :128] + part[:, 128:] * part[:, 128:]

    sq = lax.fori_loop(0, devices, square, jnp.zeros((local, 128), F32), unroll=4)
    scale = jnp.sum(sq, axis=1, keepdims=True) / samples + 1e-06
    for copy in small[1:]:
        copy.wait()
    sign = own_lab[...].astype(F32)
    bound = own_wgt[...]

    v0 = scattered(0)
    h_all[me] = (bound * sign * jnp.maximum(0.0, 1.0 - sign * v0)).astype(BF16)
    gather(h_all.at[me], h_all, ag_send.at[0], ag_recv.at[0])
    bulk(1)
    bulk(2)
    alpha0 = bound * start_ref[...]

    def permuted(vec, b):
        col = jnp.sum(onehot[b] * vec[b : b + 1], axis=1, keepdims=True)
        return jnp.broadcast_to(col, (128, 128))

    for b in range(2):
        hot = jnp.where(sub == visit_ref[b : b + 1, :], 1.0, 0.0)
        onehot_t[b] = hot.astype(BF16)
        onehot[b] = jnp.transpose(hot)
    for b in range(2):
        part = slice(128 * b, 128 * b + 128)
        yc[part] = permuted(sign, b)
        cc[part] = permuted(bound, b)
        ac[part] = permuted(alpha0, b)

    partial_gram(0)
    drain(h_all, ag_recv.at[0])
    w_col = to_col(w_row)
    stepped = w_col + contract(h_all) / (samples * scale)
    thresh = 1.0 / (4.0 * features * scale)
    primal = stepped - jnp.clip(stepped, -thresh, thresh)
    penalty = jnp.sum(jnp.abs(primal)) / (4.0 * features)
    margins(to_row(primal), 1, 0, samples // chunk)
    scatter(1)
    bulk(3)
    partial_gram(1)
    middle(0)
    v1 = scattered(1)
    loss = jnp.sum(bound * jnp.square(jnp.maximum(0.0, 1.0 - sign * v1))) / (2.0 * samples)
    obj_all[me] = jnp.full((1, 128), loss + penalty, F32)

    partial_gram(2)
    middle(1)
    partial_gram(3)
    middle(2)
    middle(3)
    pltpu.make_async_copy(fin, fin, fin_recv).wait()

    def halves(a):
        hi = a.astype(BF16)
        return hi, (a - hi.astype(F32)).astype(BF16)

    def reordered(a, b1, b2):
        hi, lo = halves(a)
        mid = jnp.dot(hi, onehot_t[b2], preferred_element_type=F32) + jnp.dot(
            lo, onehot_t[b2], preferred_element_type=F32
        )
        hi, lo = halves(mid)
        left = onehot[b1].astype(BF16)
        return jnp.dot(left, hi, preferred_element_type=F32) + jnp.dot(
            left, lo, preferred_element_type=F32
        )

    def whole(first, last):
        return own_sum[first:last] + jnp.sum(fin[:, first:last].astype(F32), axis=0)

    packed = whole(0, 128)
    turned = jnp.transpose(packed)
    diag_row = whole(256, 272)[0:1]
    first_block = jnp.where(sub > lane, packed, jnp.where(sub < lane, turned, diag_row))
    last_block = jnp.where(sub > lane, turned, packed)
    gram[0:128, 0:128] = reordered(first_block, 0, 0)
    gram[128:256, 0:128] = reordered(whole(128, 256), 1, 0)
    gram[128:256, 128:256] = reordered(last_block, 1, 1)
    for b in range(2):
        part = slice(128 * b, 128 * b + 128)
        diag = jnp.sum(jnp.where(lane == sub, gram[part, part], 0.0), axis=1, keepdims=True)
        ic[part] = jnp.broadcast_to(1.0 / (2.0 * (diag + 1e-06)), (128, 128))

    lane16 = lax.broadcasted_iota(jnp.int32, (GROUP, 128), 1)
    sub16 = lax.broadcasted_iota(jnp.int32, (GROUP, 128), 0)

    def sweep(margin):
        for b in range(2):
            mc[128 * b : 128 * b + 128] = permuted(margin, b)
        c = [jnp.zeros((1, 128), F32), jnp.zeros((1, 128), F32)]
        for t in range(rows // GROUP):
            at = slice(GROUP * t, GROUP * t + GROUP)
            b, first = t // 8, GROUP * (t % 8)
            prod = gram[at, 0:128] * c[0]
            if b:
                prod = prod + gram[at, 128:256] * c[1]
            m = mc[at] + 2.0 * jnp.sum(prod, axis=1, keepdims=True)
            old, y = ac[at], yc[at]
            new = jnp.clip(old + (1.0 - y * m) * ic[at], 0.0, cc[at])
            step = y * (new - old)
            ac[at] = new
            zc[at] = step
            c[b] = c[b] + jnp.sum(
                jnp.where(lane16 == sub16 + first, step, 0.0), axis=0, keepdims=True
            )

    def natural(col, b):
        return jnp.sum(onehot[b] * col[128 * b : 128 * b + 128], axis=0, keepdims=True)

    sweep(v1)
    for b in range(2):
        zown[b : b + 1] = natural(zc, b)
    z_all[0, me] = zown[...].astype(BF16)
    gather(z_all.at[0, me], z_all.at[0], ag_send.at[1], ag_recv.at[1])
    gather(obj_all.at[me], obj_all, obj_send, obj_recv)
    drain(z_all.at[0], ag_recv.at[1])
    first_dw = contract(z_all.at[0]) * (2.0 / devices)
    margins(to_row(first_dw), 2, 0, samples // chunk)
    scatter(2)
    v2 = v1 + scattered(2)
    sweep(v2)
    for b in range(2):
        zown[b : b + 1] = natural(zc, b)
    z_all[1, me] = zown[...].astype(BF16)
    gather(z_all.at[1, me], z_all.at[1], ag_send.at[2], ag_recv.at[2])
    for b in range(2):
        alpha_ref[b : b + 1] = natural(ac, b)
    drain(obj_all, obj_recv)
    objective_ref[...] = jnp.sum(obj_all[...], axis=0)
    for phase in range(3):
        drain(send.at[phase], rs_send.at[phase])
    drain(h_all, ag_send.at[0])
    drain(z_all.at[0], ag_send.at[1])
    drain(obj_all, obj_send)
    for b in range(4):
        bulk_wait(b, bulk_send)
        pltpu.make_async_copy(mid.at[b], mid.at[b], mid_send.at[b]).wait()
    pltpu.make_async_copy(fin, fin, fin_send).wait()
    drain(z_all.at[1], ag_recv.at[2])
    second_dw = contract(z_all.at[1]) * (2.0 / devices)
    weights_ref[...] = to_row(primal + first_dw + second_dw)
    drain(z_all.at[1], ag_send.at[2])


def solution(mesh):
    devices = mesh.shape[AXIS]

    def body(data_t, labels, sample_weight, w_start, alpha_start, visit_order):
        local, samples = data_t.shape
        per = samples // devices
        anyspace = pl.BlockSpec(memory_space=pl.ANY)
        vmem = pl.BlockSpec(memory_space=pltpu.VMEM)
        square = pltpu.VMEM((per, 128), F32)
        dma = pltpu.SemaphoreType.DMA
        weights, alpha, objective = pl.pallas_call(
            functools.partial(kernel, devices, samples),
            out_shape=(
                jax.ShapeDtypeStruct((1, local), F32),
                jax.ShapeDtypeStruct((2, 128), F32),
                jax.ShapeDtypeStruct((1, 128), F32),
            ),
            in_specs=[anyspace] * 6,
            out_specs=(vmem, vmem, vmem),
            scratch_shapes=[
                pltpu.VMEM((local, samples), BF16),
                pltpu.VMEM((2, 8, 8, local, per), BF16),
                pltpu.VMEM((4, 4, 272, 128), BF16),
                pltpu.VMEM((4, 3, 272, 128), BF16),
                pltpu.VMEM((3, 272, 128), BF16),
                pltpu.VMEM((3, 272, 128), BF16),
                pltpu.VMEM((272, 128), F32),
                pltpu.VMEM((2, 128), jnp.int32),
                pltpu.VMEM((2, 128), F32),
                pltpu.VMEM((1, local), F32),
                pltpu.VMEM((2, 128), F32),
                pltpu.VMEM((2, 128), jnp.int32),
                pltpu.VMEM((3, devices, 2, 128), F32),
                pltpu.VMEM((3, devices, 2, 128), F32),
                pltpu.VMEM((devices, 2, 128), BF16),
                pltpu.VMEM((2, devices, 2, 128), BF16),
                pltpu.VMEM((devices, 1, 128), F32),
                pltpu.VMEM((per, per), F32),
                pltpu.VMEM((2, 128, 128), F32),
                pltpu.VMEM((2, 128, 128), BF16),
                square, square, square, square, square, square,
                pltpu.VMEM((2, 128), F32),
                dma((4,)), dma((5,)), dma((2, 8)), dma((2, 4)), dma((2, 4)), dma((4,)), dma((4,)), dma, dma,
                dma((3,)), dma((3,)), dma((3,)), dma((3,)), dma, dma,
            ],
            compiler_params=pltpu.CompilerParams(collective_id=0, has_side_effects=True),
        )(
            data_t,
            labels.reshape(devices, 2, 128),
            sample_weight.reshape(devices, 2, 128),
            w_start.reshape(1, local),
            alpha_start.reshape(2, 128),
            visit_order,
        )
        return weights.reshape(local), alpha.reshape(per), objective[0, 0]

    return jax.shard_map(
        body,
        mesh=mesh,
        in_specs=(P(AXIS, None), P(), P(), P(AXIS), P(AXIS), P(AXIS, None)),
        out_specs=(P(AXIS), P(AXIS), P()),
        check_vma=False,
    )
```

```python
import functools

import jax
import jax.numpy as jnp
from jax import lax
from jax.experimental import pallas as pl
from jax.experimental.pallas import tpu as pltpu
from jax.sharding import PartitionSpec as P

F32 = jnp.float32
BF16 = jnp.bfloat16
MESH = pl.DeviceIdType.MESH
AXIS = "shard"
GROUP = 16
ORDER = (2, 1, 3, 0)


def kernel(devices, samples, x_hbm, lab_hbm, wgt_hbm, w_hbm, start_hbm, visit_hbm,
           result_ref,
           x, raw, pout, mid, psum, fin, own_sum, own_lab, own_wgt, w_ref, start_ref, visit_ref,
           send, recv, h_all, z_all, obj_all,
           gram, onehot, onehot_t, mc, yc, lc, cc, ac, ic, zc, zown,
           load_sem, small_sem, own_sem, bulk_send, bulk_recv, mid_send, mid_recv, fin_send, fin_recv,
           rs_send, rs_recv, ag_send, ag_recv, obj_send, obj_recv):
    me = lax.axis_index(AXIS)
    local = x.shape[0]
    features = local * devices
    rows = 256
    others = devices - 1

    my_z, my_x, my_y, my_c = me // 32, lax.rem(me // 8, 4), lax.rem(me // 2, 4), lax.rem(me, 2)
    near = [
        lax.rem(my_y + dy, 4) * 2 + lax.rem(my_c + dc, 2)
        for dy in (2, 1, 3, 0)
        for dc in (1, 0)
    ]

    def peers(visit):
        def one(i, carry):
            base = (
                lax.rem(my_z + 2 + i // 4, 4) * 32 + lax.rem(my_x + 2 + lax.rem(i, 4), 4) * 8
            )
            for place in near:
                visit(base + place)
            return carry

        lax.fori_loop(0, 10, one, 0)
        lax.fori_loop(11, 16, one, 0)
        for place in near[:7]:
            visit(my_z * 32 + my_x * 8 + place)

    barrier = pltpu.get_barrier_semaphore()

    def greet(to):
        pl.semaphore_signal(barrier, inc=1, device_id=(to,), device_id_type=MESH)

    pieces = load_sem.shape[0]
    width = samples // pieces

    def load(i):
        at = pl.ds(i * width, width)
        return pltpu.make_async_copy(x_hbm.at[:, at], x.at[:, at], load_sem.at[i])

    small = [
        pltpu.make_async_copy(src, dst, small_sem.at[i])
        for i, (src, dst) in enumerate(
            (
                (w_hbm, w_ref),
                (lab_hbm.at[me], own_lab),
                (wgt_hbm.at[me], own_wgt),
                (start_hbm, start_ref),
                (visit_hbm, visit_ref),
            )
        )
    ]
    small[0].start()
    for i in range(pieces):
        load(i).start()
    peers(greet)
    for copy in small[1:]:
        copy.start()

    def slice_of(to):
        return pl.ds(pl.multiple_of(to * rows, rows), rows)

    def device(z, xx, y, core):
        return ((z * 4 + xx) * 4 + y) * 2 + core

    def line_of(entry):
        return entry % 3 if entry < 12 else (entry - 12) // 2

    def owner_of(entry, place, core):
        line = line_of(entry)
        if entry >= 12:
            y = entry - 12
            other = lax.rem(11 - place - y, 4)
            return device(place, other, y, core) if line == 0 else device(other, place, y, core)
        away = ORDER[entry // 3]
        if line == 2:
            z = lax.rem(my_z + away, 4)
            return device(z, lax.rem(10 - z - place, 4), place, core)
        y = lax.rem(my_y + away, 4)
        other = lax.rem(8 + line - place - y, 4)
        return device(place, other, y, core) if line == 0 else device(other, place, y, core)

    def collector(line, place, core):
        at = [my_z, my_x, my_y]
        at[line] = place
        return device(*at, core)

    my_place = (my_z, my_x, my_y)

    def entries(b):
        return range(12, 16) if b == 4 else range(3 * b, 3 * b + 3)

    def own_slices(b):
        return [
            pltpu.make_async_copy(
                x_hbm.at[:, slice_of(owner_of(e, my_place[line_of(e)], my_c))],
                raw.at[e, my_place[line_of(e)] * 2 + my_c],
                own_sem.at[e],
            )
            for e in entries(b)
        ]

    def bulk(b):
        for step, other in ((1, 0), (3, 0), (2, 1), (0, 1), (1, 1), (3, 1), (2, 0)):
            for e in entries(b):
                line = line_of(e)
                place = lax.rem(my_place[line] + step, 4)
                core = lax.rem(my_c + other, 2)
                pltpu.make_async_remote_copy(
                    src_ref=x.at[:, slice_of(owner_of(e, place, core))],
                    dst_ref=raw.at[e, my_place[line] * 2 + my_c],
                    send_sem=bulk_send.at[b], recv_sem=bulk_recv.at[b],
                    device_id=(collector(line, place, core),), device_id_type=MESH,
                ).start()

    def bulk_wait(b, sem):
        part = entries(b)
        slots = raw.at[pl.ds(part[0], len(part)), pl.ds(0, 7)]
        pltpu.make_async_copy(slots, slots, sem.at[b]).wait()

    lane = lax.broadcasted_iota(jnp.int32, (128, 128), 1)
    sub = lax.broadcasted_iota(jnp.int32, (128, 128), 0)

    def push(entry, j, slot, z, y):
        pltpu.make_async_remote_copy(
            src_ref=pout.at[entry], dst_ref=mid.at[j, slot],
            send_sem=mid_send.at[j], recv_sem=mid_recv.at[j],
            device_id=(device(z, my_x, y, my_c),), device_id_type=MESH,
        ).start()

    def partial_gram(b):
        for copy in own_slices(b):
            copy.wait()
        bulk_wait(b, bulk_recv)
        for e in entries(b):
            piece = raw[e].reshape(8 * local, rows)
            full = lax.dot_general(
                piece, piece, (((0,), (0,)), ((), ())), preferred_element_type=F32
            )
            first, last = full[:128, :128], full[128:, 128:]
            pout[e, 0:128] = jnp.where(sub > lane, first, last).astype(BF16)
            pout[e, 128:256] = full[128:, :128].astype(BF16)
            diag = jnp.sum(jnp.where(sub == lane, first, 0.0), axis=0, keepdims=True)
            pout[e, 256:272] = jnp.broadcast_to(diag, (16, 128)).astype(BF16)
            if e < 9:
                away = ORDER[e // 3]
                if line_of(e) == 2:
                    push(e, 2, e // 3, lax.rem(my_z + away, 4), my_y)
                else:
                    push(e, line_of(e), e // 3, my_z, lax.rem(my_y + away, 4))
        if b == 4:
            for dy in (2, 1, 3):
                y = lax.rem(my_y + dy, 4)
                push(12 + y, 3, dy - 1, my_z, y)

    def middle(j):
        pltpu.make_async_copy(mid.at[j], mid.at[j], mid_recv.at[j]).wait()
        own = pout[9 + j] if j < 3 else pout[12 + my_y]
        total = own.astype(F32) + jnp.sum(mid[j].astype(F32), axis=0)
        along_x = lax.rem(8 + j - my_z - my_y, 4)
        along_z = lax.rem(8 + j - my_x - my_y, 4)
        turn = {0: 0, 1: 1, 2: 0, 3: my_y // 2}[j]
        z = my_z * (1 - turn) + along_z * turn
        xx = along_x * (1 - turn) + my_x * turn
        slot = lax.rem(z - my_z + xx - my_x + 4, 4) - 1
        mine = lax.rem(my_z + my_x + my_y, 4) == j

        @pl.when(mine)
        def _():
            own_sum[...] = total

        @pl.when(jnp.logical_not(mine))
        def _():
            psum[j] = total.astype(BF16)
            pltpu.make_async_remote_copy(
                src_ref=psum.at[j], dst_ref=fin.at[slot],
                send_sem=fin_send, recv_sem=fin_recv,
                device_id=(device(z, xx, my_y, my_c),), device_id_type=MESH,
            ).start()

    for b in (4, 0, 1, 2, 3):
        for copy in own_slices(b):
            copy.start()

    eye = lax.broadcasted_iota(jnp.int32, (local, local), 0) == lax.broadcasted_iota(
        jnp.int32, (local, local), 1
    )

    def to_row(col):
        return jnp.sum(jnp.where(eye, col, 0.0), axis=0, keepdims=True)

    def to_col(row):
        return jnp.sum(jnp.where(eye, row, 0.0), axis=1, keepdims=True)

    chunk = samples // 4

    def margins(row, phase, first, last):
        lhs = jnp.broadcast_to(row, (8, local)).astype(BF16)

        def one(i, carry):
            out = jnp.dot(
                lhs, x[:, pl.ds(pl.multiple_of(i * chunk, chunk), chunk)],
                preferred_element_type=F32,
            )
            for j in range(chunk // 128):
                send[phase, i * (chunk // rows) + j // 2, j % 2 : j % 2 + 1, :] = out[
                    0:1, 128 * j : 128 * j + 128
                ]
            return carry

        lax.fori_loop(first, last, one, 0)

    def scatter(phase):
        def one(to):
            pltpu.make_async_remote_copy(
                src_ref=send.at[phase, to], dst_ref=recv.at[phase, me],
                send_sem=rs_send.at[phase], recv_sem=rs_recv.at[phase],
                device_id=(to,), device_id_type=MESH,
            ).start()

        recv[phase, me] = send[phase, me]
        peers(one)

    def scattered(phase):
        many = recv.at[phase, pl.ds(0, others)]
        pltpu.make_async_copy(many, many, rs_recv.at[phase]).wait()
        return jnp.sum(recv[phase], axis=0)

    def gather(src, buf, send_sem, recv_sem):
        def one(to):
            pltpu.make_async_remote_copy(
                src_ref=src, dst_ref=buf.at[me],
                send_sem=send_sem, recv_sem=recv_sem,
                device_id=(to,), device_id_type=MESH,
            ).start()

        peers(one)

    def drain(buf, sem):
        many = buf.at[pl.ds(0, others)]
        pltpu.make_async_copy(many, many, sem).wait()

    def contract(buf):
        def one(d, acc):
            part = x[:, pl.ds(pl.multiple_of(d * rows, rows), rows)].astype(F32)
            v = buf[d].astype(F32)
            return acc + part[:, :128] * v[0:1] + part[:, 128:] * v[1:2]

        acc = lax.fori_loop(0, devices, one, jnp.zeros((local, 128), F32), unroll=4)
        return jnp.sum(acc, axis=1, keepdims=True)

    small[0].wait()
    w_row = w_ref[...]
    per = width // chunk
    for i in range(pieces):
        load(i).wait()
        margins(w_row, 0, i * per, (i + 1) * per)
    pl.semaphore_wait(barrier, others)
    scatter(0)
    bulk(4)
    bulk(0)
    bulk(1)

    def square(d, acc):
        part = x[:, pl.ds(pl.multiple_of(d * rows, rows), rows)].astype(F32)
        return acc + part[:, :128] * part[:, :128] + part[:, 128:] * part[:, 128:]

    sq = lax.fori_loop(0, devices, square, jnp.zeros((local, 128), F32), unroll=4)
    scale = jnp.sum(sq, axis=1, keepdims=True) / samples + 1e-06
    for copy in small[1:]:
        copy.wait()
    sign = own_lab[...].astype(F32)
    bound = own_wgt[...]

    v0 = scattered(0)
    h_all[me] = (bound * sign * jnp.maximum(0.0, 1.0 - sign * v0)).astype(BF16)
    gather(h_all.at[me], h_all, ag_send.at[0], ag_recv.at[0])
    bulk(2)
    bulk(3)
    alpha0 = bound * start_ref[...]

    def permuted(vec, b):
        col = jnp.sum(onehot[b] * vec[b : b + 1], axis=1, keepdims=True)
        return jnp.broadcast_to(col, (128, 128))

    for b in range(2):
        hot = jnp.where(sub == visit_ref[b : b + 1, :], 1.0, 0.0)
        onehot_t[b] = hot.astype(BF16)
        onehot[b] = jnp.transpose(hot)
    for b in range(2):
        part = slice(128 * b, 128 * b + 128)
        yc[part] = permuted(sign, b)
        edge = yc[part] * permuted(bound, b)
        lc[part] = jnp.minimum(edge, 0.0)
        cc[part] = jnp.maximum(edge, 0.0)
        ac[part] = yc[part] * permuted(alpha0, b)

    partial_gram(4)
    partial_gram(0)
    partial_gram(1)
    drain(h_all, ag_recv.at[0])
    w_col = to_col(w_row)
    stepped = w_col + contract(h_all) / (samples * scale)
    thresh = 1.0 / (4.0 * features * scale)
    primal = stepped - jnp.clip(stepped, -thresh, thresh)
    penalty = jnp.sum(jnp.abs(primal)) / (4.0 * features)
    margins(to_row(primal), 1, 0, samples // chunk)
    scatter(1)
    partial_gram(2)
    partial_gram(3)
    middle(3)
    middle(0)
    middle(1)
    middle(2)
    v1 = scattered(1)
    loss = jnp.sum(bound * jnp.square(jnp.maximum(0.0, 1.0 - sign * v1))) / (2.0 * samples)
    obj_all[me] = jnp.full((1, 128), loss + penalty, F32)

    pltpu.make_async_copy(fin, fin, fin_recv).wait()

    def halves(a):
        hi = a.astype(BF16)
        return hi, (a - hi.astype(F32)).astype(BF16)

    def reordered(a, b1, b2):
        hi, lo = halves(a)
        mid = jnp.dot(hi, onehot_t[b2], preferred_element_type=F32) + jnp.dot(
            lo, onehot_t[b2], preferred_element_type=F32
        )
        hi, lo = halves(mid)
        left = onehot[b1].astype(BF16)
        return jnp.dot(left, hi, preferred_element_type=F32) + jnp.dot(
            left, lo, preferred_element_type=F32
        )

    def whole(first, last):
        return own_sum[first:last] + jnp.sum(fin[:, first:last].astype(F32), axis=0)

    packed = whole(0, 128)
    turned = jnp.transpose(packed)
    diag_row = whole(256, 272)[0:1]
    first_block = jnp.where(sub > lane, packed, jnp.where(sub < lane, turned, diag_row))
    last_block = jnp.where(sub > lane, turned, packed)
    gram[0:128, 0:128] = reordered(first_block, 0, 0)
    gram[128:256, 0:128] = reordered(whole(128, 256), 1, 0)
    gram[128:256, 128:256] = reordered(last_block, 1, 1)
    for b in range(2):
        part = slice(128 * b, 128 * b + 128)
        diag = jnp.sum(jnp.where(lane == sub, gram[part, part], 0.0), axis=1, keepdims=True)
        ic[part] = jnp.broadcast_to(1.0 / (2.0 * (diag + 1e-06)), (128, 128))

    lane16 = lax.broadcasted_iota(jnp.int32, (GROUP, 128), 1)
    sub16 = lax.broadcasted_iota(jnp.int32, (GROUP, 128), 0)

    def sweep(margin):
        for b in range(2):
            part = slice(128 * b, 128 * b + 128)
            mc[part] = ac[part] + (yc[part] - permuted(margin, b)) * ic[part]
        c = [jnp.zeros((1, 128), F32), jnp.zeros((1, 128), F32)]
        for t in range(rows // GROUP):
            at = slice(GROUP * t, GROUP * t + GROUP)
            b, first = t // 8, GROUP * (t % 8)
            aim = mc[at]
            if t:
                prod = gram[at, 0:128] * c[0]
                if b:
                    prod = prod + gram[at, 128:256] * c[1]
                aim = aim - 2.0 * ic[at] * jnp.sum(prod, axis=1, keepdims=True)
            new = jnp.minimum(jnp.maximum(aim, lc[at]), cc[at])
            step = new - ac[at]
            ac[at] = new
            zc[at] = step
            c[b] = c[b] + jnp.sum(
                jnp.where(lane16 == sub16 + first, step, 0.0), axis=0, keepdims=True
            )

    def natural(col, b):
        return jnp.sum(onehot[b] * col[128 * b : 128 * b + 128], axis=0, keepdims=True)

    sweep(v1)
    for b in range(2):
        zown[b : b + 1] = natural(zc, b)
    z_all[0, me] = zown[...].astype(BF16)
    gather(z_all.at[0, me], z_all.at[0], ag_send.at[1], ag_recv.at[1])
    gather(obj_all.at[me], obj_all, obj_send, obj_recv)
    drain(z_all.at[0], ag_recv.at[1])
    first_dw = contract(z_all.at[0]) * (2.0 / devices)
    margins(to_row(first_dw), 2, 0, samples // chunk)
    scatter(2)
    v2 = v1 + scattered(2)
    sweep(v2)
    for b in range(2):
        zown[b : b + 1] = natural(zc, b)
    z_all[1, me] = zown[...].astype(BF16)
    gather(z_all.at[1, me], z_all.at[1], ag_send.at[2], ag_recv.at[2])
    for b in range(2):
        result_ref[1 + b : 2 + b] = sign[b : b + 1] * natural(ac, b)
    drain(obj_all, obj_recv)
    result_ref[3:4] = jnp.sum(obj_all[...], axis=0)
    for phase in range(3):
        drain(send.at[phase], rs_send.at[phase])
    drain(h_all, ag_send.at[0])
    drain(z_all.at[0], ag_send.at[1])
    drain(obj_all, obj_send)
    for b in range(5):
        bulk_wait(b, bulk_send)
    for j in range(4):
        pltpu.make_async_copy(mid.at[j], mid.at[j], mid_send.at[j]).wait()
    pltpu.make_async_copy(fin, fin, fin_send).wait()
    drain(z_all.at[1], ag_recv.at[2])
    second_dw = contract(z_all.at[1]) * (2.0 / devices)
    result_ref[0:1, :local] = to_row(primal + first_dw + second_dw)
    drain(z_all.at[1], ag_send.at[2])


def finish(result, weights, alpha, objective):
    weights[...] = result[0:1, : weights.shape[1]]
    alpha[...] = result[1:3]
    objective[...] = result[3:4]


def solution(mesh):
    devices = mesh.shape[AXIS]

    def body(data_t, labels, sample_weight, w_start, alpha_start, visit_order):
        local, samples = data_t.shape
        per = samples // devices
        anyspace = pl.BlockSpec(memory_space=pl.ANY)
        vmem = pl.BlockSpec(memory_space=pltpu.VMEM)
        square = pltpu.VMEM((per, 128), F32)
        dma = pltpu.SemaphoreType.DMA
        result = pl.pallas_call(
            functools.partial(kernel, devices, samples),
            out_shape=jax.ShapeDtypeStruct((4, 128), F32),
            in_specs=[anyspace] * 6,
            out_specs=vmem,
            scratch_shapes=[
                pltpu.VMEM((local, samples), BF16),
                pltpu.VMEM((16, 8, local, per), BF16),
                pltpu.VMEM((16, 272, 128), BF16),
                pltpu.VMEM((4, 3, 272, 128), BF16),
                pltpu.VMEM((4, 272, 128), BF16),
                pltpu.VMEM((3, 272, 128), BF16),
                pltpu.VMEM((272, 128), F32),
                pltpu.VMEM((2, 128), jnp.int32),
                pltpu.VMEM((2, 128), F32),
                pltpu.VMEM((1, local), F32),
                pltpu.VMEM((2, 128), F32),
                pltpu.VMEM((2, 128), jnp.int32),
                pltpu.VMEM((3, devices, 2, 128), F32),
                pltpu.VMEM((3, devices, 2, 128), F32),
                pltpu.VMEM((devices, 2, 128), BF16),
                pltpu.VMEM((2, devices, 2, 128), BF16),
                pltpu.VMEM((devices, 1, 128), F32),
                pltpu.VMEM((per, per), F32),
                pltpu.VMEM((2, 128, 128), F32),
                pltpu.VMEM((2, 128, 128), BF16),
                *[square] * 7,
                pltpu.VMEM((2, 128), F32),
                dma((4,)), dma((5,)), dma((16,)), dma((5,)), dma((5,)), dma((4,)), dma((4,)), dma, dma,
                dma((3,)), dma((3,)), dma((3,)), dma((3,)), dma, dma,
            ],
            compiler_params=pltpu.CompilerParams(
                collective_id=0, has_side_effects=True, vmem_limit_bytes=61998 * 1024
            ),
        )(
            data_t,
            labels.reshape(devices, 2, 128),
            sample_weight.reshape(devices, 2, 128),
            w_start.reshape(1, local),
            alpha_start.reshape(2, 128),
            visit_order,
        )
        weights, alpha, objective = pl.pallas_call(
            finish,
            out_shape=(
                jax.ShapeDtypeStruct((1, local), F32),
                jax.ShapeDtypeStruct((2, 128), F32),
                jax.ShapeDtypeStruct((1, 128), F32),
            ),
            in_specs=[vmem],
            out_specs=(vmem,) * 3,
            compiler_params=pltpu.CompilerParams(vmem_limit_bytes=1024 * 1024),
        )(result)
        return weights.reshape(local), alpha.reshape(per), objective[0, 0]

    return jax.shard_map(
        body,
        mesh=mesh,
        in_specs=(P(AXIS, None), P(), P(), P(AXIS), P(AXIS), P(AXIS, None)),
        out_specs=(P(AXIS), P(AXIS), P()),
        check_vma=False,
    )
```

```python
import functools

import jax
import jax.numpy as jnp
from jax import lax
from jax.experimental import pallas as pl
from jax.experimental.pallas import tpu as pltpu
from jax.sharding import PartitionSpec as P

F32 = jnp.float32
BF16 = jnp.bfloat16
MESH = pl.DeviceIdType.MESH
AXIS = "shard"
GROUP = 16
ORDER = (2, 1, 3, 0)


def kernel(devices, samples, x_hbm, lab_hbm, wgt_hbm, w_hbm, start_hbm, visit_hbm,
           result_ref,
           x, raw, pout, mid, psum, fin, own_sum, own_lab, own_wgt, w_ref, start_ref, visit_ref,
           send, recv, h_all, z_all, obj_all,
           gram, onehot, onehot_t, mc, yc, lc, cc, ac, ic, zc, zown,
           load_sem, small_sem, own_sem, bulk_send, bulk_recv, mid_send, mid_recv, fin_send, fin_recv,
           rs_send, rs_recv, ag_send, ag_recv, obj_send, obj_recv):
    me = lax.axis_index(AXIS)
    local = x.shape[0]
    features = local * devices
    rows = 256
    others = devices - 1

    my_z, my_x, my_y, my_c = me // 32, lax.rem(me // 8, 4), lax.rem(me // 2, 4), lax.rem(me, 2)
    near = [
        lax.rem(my_y + dy, 4) * 2 + lax.rem(my_c + dc, 2)
        for dy in (2, 1, 3, 0)
        for dc in (1, 0)
    ]

    def plane(dz, visit):
        z = lax.rem(my_z + dz, 4)

        def one(dx, carry):
            for place in near:
                visit(z * 32 + lax.rem(my_x + dx, 4) * 8 + place)
            return carry

        if dz:
            lax.fori_loop(2, 6, one, 0)
        else:
            lax.fori_loop(1, 4, one, 0)
            for place in near[:7]:
                visit(z * 32 + my_x * 8 + place)

    PLANES = (2, 1, 3, 0)

    def peers(visit):
        for dz in PLANES:
            plane(dz, visit)

    barrier = pltpu.get_barrier_semaphore()

    def greet(to):
        pl.semaphore_signal(barrier, inc=1, device_id=(to,), device_id_type=MESH)

    pieces = load_sem.shape[0]
    width = samples // pieces

    def load(i):
        at = pl.ds(i * width, width)
        return pltpu.make_async_copy(x_hbm.at[:, at], x.at[:, at], load_sem.at[i])

    small = [
        pltpu.make_async_copy(src, dst, small_sem.at[i])
        for i, (src, dst) in enumerate(
            (
                (w_hbm, w_ref),
                (lab_hbm.at[me], own_lab),
                (wgt_hbm.at[me], own_wgt),
                (start_hbm, start_ref),
                (visit_hbm, visit_ref),
            )
        )
    ]
    small[0].start()
    for i in range(pieces):
        load(i).start()
    peers(greet)
    for copy in small[1:]:
        copy.start()

    def slice_of(to):
        return pl.ds(pl.multiple_of(to * rows, rows), rows)

    def device(z, xx, y, core):
        return ((z * 4 + xx) * 4 + y) * 2 + core

    def line_of(entry):
        return entry % 3 if entry < 12 else (entry - 12) // 2

    def owner_of(entry, place, core):
        line = line_of(entry)
        if entry >= 12:
            y = entry - 12
            other = lax.rem(11 - place - y, 4)
            return device(place, other, y, core) if line == 0 else device(other, place, y, core)
        away = ORDER[entry // 3]
        if line == 2:
            z = lax.rem(my_z + away, 4)
            return device(z, lax.rem(10 - z - place, 4), place, core)
        y = lax.rem(my_y + away, 4)
        other = lax.rem(8 + line - place - y, 4)
        return device(place, other, y, core) if line == 0 else device(other, place, y, core)

    def collector(line, place, core):
        at = [my_z, my_x, my_y]
        at[line] = place
        return device(*at, core)

    my_place = (my_z, my_x, my_y)

    def entries(b):
        return range(12, 16) if b == 4 else range(3 * b, 3 * b + 3)

    def own_slices(b):
        return [
            pltpu.make_async_copy(
                x_hbm.at[:, slice_of(owner_of(e, my_place[line_of(e)], my_c))],
                raw.at[e, my_place[line_of(e)] * 2 + my_c],
                own_sem.at[e],
            )
            for e in entries(b)
        ]

    def bulk(b):
        for step, other in ((1, 0), (3, 0), (2, 1), (0, 1), (1, 1), (3, 1), (2, 0)):
            for e in entries(b):
                line = line_of(e)
                place = lax.rem(my_place[line] + step, 4)
                core = lax.rem(my_c + other, 2)
                pltpu.make_async_remote_copy(
                    src_ref=x.at[:, slice_of(owner_of(e, place, core))],
                    dst_ref=raw.at[e, my_place[line] * 2 + my_c],
                    send_sem=bulk_send.at[b], recv_sem=bulk_recv.at[b],
                    device_id=(collector(line, place, core),), device_id_type=MESH,
                ).start()

    def bulk_wait(b, sem):
        part = entries(b)
        slots = raw.at[pl.ds(part[0], len(part)), pl.ds(0, 7)]
        pltpu.make_async_copy(slots, slots, sem.at[b]).wait()

    lane = lax.broadcasted_iota(jnp.int32, (128, 128), 1)
    sub = lax.broadcasted_iota(jnp.int32, (128, 128), 0)

    def push(entry, j, slot, z, y):
        pltpu.make_async_remote_copy(
            src_ref=pout.at[entry], dst_ref=mid.at[j, slot],
            send_sem=mid_send.at[j], recv_sem=mid_recv.at[j],
            device_id=(device(z, my_x, y, my_c),), device_id_type=MESH,
        ).start()

    def partial_gram(b):
        for copy in own_slices(b):
            copy.wait()
        bulk_wait(b, bulk_recv)
        for e in entries(b):
            piece = raw[e].reshape(8 * local, rows)
            full = lax.dot_general(
                piece, piece, (((0,), (0,)), ((), ())), preferred_element_type=F32
            )
            first, last = full[:128, :128], full[128:, 128:]
            pout[e, 0:128] = jnp.where(sub > lane, first, last).astype(BF16)
            pout[e, 128:256] = full[128:, :128].astype(BF16)
            diag = jnp.sum(jnp.where(sub == lane, first, 0.0), axis=0, keepdims=True)
            pout[e, 256:272] = jnp.broadcast_to(diag, (16, 128)).astype(BF16)
            if e < 9:
                away = ORDER[e // 3]
                if line_of(e) == 2:
                    push(e, 2, e // 3, lax.rem(my_z + away, 4), my_y)
                else:
                    push(e, line_of(e), e // 3, my_z, lax.rem(my_y + away, 4))
        if b == 4:
            for dy in (2, 1, 3):
                y = lax.rem(my_y + dy, 4)
                push(12 + y, 3, dy - 1, my_z, y)

    def middle(j):
        pltpu.make_async_copy(mid.at[j], mid.at[j], mid_recv.at[j]).wait()
        own = pout[9 + j] if j < 3 else pout[12 + my_y]
        total = own.astype(F32) + jnp.sum(mid[j].astype(F32), axis=0)
        along_x = lax.rem(8 + j - my_z - my_y, 4)
        along_z = lax.rem(8 + j - my_x - my_y, 4)
        turn = {0: 0, 1: 1, 2: 0, 3: my_y // 2}[j]
        z = my_z * (1 - turn) + along_z * turn
        xx = along_x * (1 - turn) + my_x * turn
        slot = lax.rem(z - my_z + xx - my_x + 4, 4) - 1
        mine = lax.rem(my_z + my_x + my_y, 4) == j

        @pl.when(mine)
        def _():
            own_sum[...] = total

        @pl.when(jnp.logical_not(mine))
        def _():
            psum[j] = total.astype(BF16)
            pltpu.make_async_remote_copy(
                src_ref=psum.at[j], dst_ref=fin.at[slot],
                send_sem=fin_send, recv_sem=fin_recv,
                device_id=(device(z, xx, my_y, my_c),), device_id_type=MESH,
            ).start()

    for b in (4, 0, 1, 2, 3):
        for copy in own_slices(b):
            copy.start()

    eye = lax.broadcasted_iota(jnp.int32, (local, local), 0) == lax.broadcasted_iota(
        jnp.int32, (local, local), 1
    )

    def to_row(col):
        return jnp.sum(jnp.where(eye, col, 0.0), axis=0, keepdims=True)

    def to_col(row):
        return jnp.sum(jnp.where(eye, row, 0.0), axis=1, keepdims=True)

    chunk = samples // 4

    def margins(row, phase, first, last):
        lhs = jnp.broadcast_to(row, (8, local)).astype(BF16)

        def one(i, carry):
            out = jnp.dot(
                lhs, x[:, pl.ds(pl.multiple_of(i * chunk, chunk), chunk)],
                preferred_element_type=F32,
            )
            for j in range(chunk // 128):
                send[phase, i * (chunk // rows) + j // 2, j % 2 : j % 2 + 1, :] = out[
                    0:1, 128 * j : 128 * j + 128
                ]
            return carry

        lax.fori_loop(first, last, one, 0)

    def scatter(phase, before):
        def one(to):
            pltpu.make_async_remote_copy(
                src_ref=send.at[phase, to], dst_ref=recv.at[phase, me],
                send_sem=rs_send.at[phase], recv_sem=rs_recv.at[phase],
                device_id=(to,), device_id_type=MESH,
            ).start()

        for dz in PLANES:
            before(lax.rem(my_z + dz, 4))
            plane(dz, one)
        recv[phase, me] = send[phase, me]

    def margins_scatter(row, phase):
        scatter(phase, lambda z: margins(row, phase, z, z + 1))

    def scattered(phase):
        many = recv.at[phase, pl.ds(0, others)]
        pltpu.make_async_copy(many, many, rs_recv.at[phase]).wait()
        return jnp.sum(recv[phase], axis=0)

    def gather(src, buf, send_sem, recv_sem):
        for dz in PLANES:

            def one(to):
                pltpu.make_async_remote_copy(
                    src_ref=src, dst_ref=buf.at[me],
                    send_sem=send_sem, recv_sem=recv_sem.at[dz],
                    device_id=(to,), device_id_type=MESH,
                ).start()

            plane(dz, one)

    def arrived(buf, sem, dz):
        many = buf.at[pl.ds(0, devices // 4 - (dz == 0))]
        pltpu.make_async_copy(many, many, sem.at[dz]).wait()

    def drain(buf, sem):
        many = buf.at[pl.ds(0, others)]
        pltpu.make_async_copy(many, many, sem).wait()

    def contract(buf, sem):
        acc = jnp.zeros((local, 128), F32)
        for dz in PLANES[::-1]:
            arrived(buf, sem, dz)
            first = lax.rem(my_z + 4 - dz, 4) * 32

            def one(i, acc):
                d = first + i
                part = x[:, pl.ds(pl.multiple_of(d * rows, rows), rows)].astype(F32)
                v = buf[d].astype(F32)
                return acc + part[:, :128] * v[0:1] + part[:, 128:] * v[1:2]

            acc = lax.fori_loop(0, 32, one, acc, unroll=4)
        return jnp.sum(acc, axis=1, keepdims=True)

    small[0].wait()
    w_row = w_ref[...]
    per = width // chunk
    for i in range(pieces):
        load(i).wait()
        margins(w_row, 0, i * per, (i + 1) * per)
    pl.semaphore_wait(barrier, others)
    scatter(0, lambda z: None)
    bulk(4)
    bulk(0)
    bulk(1)

    def square(d, acc):
        part = x[:, pl.ds(pl.multiple_of(d * rows, rows), rows)].astype(F32)
        return acc + part[:, :128] * part[:, :128] + part[:, 128:] * part[:, 128:]

    sq = lax.fori_loop(0, devices, square, jnp.zeros((local, 128), F32), unroll=4)
    scale = jnp.sum(sq, axis=1, keepdims=True) / samples + 1e-06
    for copy in small[1:]:
        copy.wait()
    sign = own_lab[...].astype(F32)
    bound = own_wgt[...]

    v0 = scattered(0)
    h_all[me] = (bound * sign * jnp.maximum(0.0, 1.0 - sign * v0)).astype(BF16)
    gather(h_all.at[me], h_all, ag_send.at[0], ag_recv.at[0])
    bulk(2)
    bulk(3)
    alpha0 = bound * start_ref[...]

    def permuted(vec, b):
        col = jnp.sum(onehot[b] * vec[b : b + 1], axis=1, keepdims=True)
        return jnp.broadcast_to(col, (128, 128))

    for b in range(2):
        hot = jnp.where(sub == visit_ref[b : b + 1, :], 1.0, 0.0)
        onehot_t[b] = hot.astype(BF16)
        onehot[b] = jnp.transpose(hot)
    for b in range(2):
        part = slice(128 * b, 128 * b + 128)
        yc[part] = permuted(sign, b)
        edge = yc[part] * permuted(bound, b)
        lc[part] = jnp.minimum(edge, 0.0)
        cc[part] = jnp.maximum(edge, 0.0)
        ac[part] = yc[part] * permuted(alpha0, b)

    partial_gram(4)
    partial_gram(0)
    partial_gram(1)
    w_col = to_col(w_row)
    stepped = w_col + contract(h_all, ag_recv.at[0]) / (samples * scale)
    thresh = 1.0 / (4.0 * features * scale)
    primal = stepped - jnp.clip(stepped, -thresh, thresh)
    penalty = jnp.sum(jnp.abs(primal)) / (4.0 * features)
    margins_scatter(to_row(primal), 1)
    partial_gram(2)
    partial_gram(3)
    middle(3)
    middle(0)
    middle(1)
    middle(2)
    v1 = scattered(1)
    loss = jnp.sum(bound * jnp.square(jnp.maximum(0.0, 1.0 - sign * v1))) / (2.0 * samples)
    obj_all[me] = jnp.full((1, 128), loss + penalty, F32)

    pltpu.make_async_copy(fin, fin, fin_recv).wait()

    def halves(a):
        hi = a.astype(BF16)
        return hi, (a - hi.astype(F32)).astype(BF16)

    def reordered(a, b1, b2):
        hi, lo = halves(a)
        mid = jnp.dot(hi, onehot_t[b2], preferred_element_type=F32) + jnp.dot(
            lo, onehot_t[b2], preferred_element_type=F32
        )
        hi, lo = halves(mid)
        left = onehot[b1].astype(BF16)
        return jnp.dot(left, hi, preferred_element_type=F32) + jnp.dot(
            left, lo, preferred_element_type=F32
        )

    def whole(first, last):
        return own_sum[first:last] + jnp.sum(fin[:, first:last].astype(F32), axis=0)

    packed = whole(0, 128)
    turned = jnp.transpose(packed)
    diag_row = whole(256, 272)[0:1]
    first_block = jnp.where(sub > lane, packed, jnp.where(sub < lane, turned, diag_row))
    last_block = jnp.where(sub > lane, turned, packed)
    gram[0:128, 0:128] = reordered(first_block, 0, 0)
    gram[128:256, 0:128] = reordered(whole(128, 256), 1, 0)
    gram[128:256, 128:256] = reordered(last_block, 1, 1)
    for b in range(2):
        part = slice(128 * b, 128 * b + 128)
        diag = jnp.sum(jnp.where(lane == sub, gram[part, part], 0.0), axis=1, keepdims=True)
        ic[part] = jnp.broadcast_to(1.0 / (2.0 * (diag + 1e-06)), (128, 128))

    lane16 = lax.broadcasted_iota(jnp.int32, (GROUP, 128), 1)
    sub16 = lax.broadcasted_iota(jnp.int32, (GROUP, 128), 0)

    def sweep(margin):
        for b in range(2):
            part = slice(128 * b, 128 * b + 128)
            mc[part] = ac[part] + (yc[part] - permuted(margin, b)) * ic[part]
        c = [jnp.zeros((1, 128), F32), jnp.zeros((1, 128), F32)]
        for t in range(rows // GROUP):
            at = slice(GROUP * t, GROUP * t + GROUP)
            b, first = t // 8, GROUP * (t % 8)
            aim = mc[at]
            if t:
                prod = gram[at, 0:128] * c[0]
                if b:
                    prod = prod + gram[at, 128:256] * c[1]
                aim = aim - 2.0 * ic[at] * jnp.sum(prod, axis=1, keepdims=True)
            new = jnp.minimum(jnp.maximum(aim, lc[at]), cc[at])
            step = new - ac[at]
            ac[at] = new
            zc[at] = step
            c[b] = c[b] + jnp.sum(
                jnp.where(lane16 == sub16 + first, step, 0.0), axis=0, keepdims=True
            )

    def natural(col, b):
        return jnp.sum(onehot[b] * col[128 * b : 128 * b + 128], axis=0, keepdims=True)

    sweep(v1)
    for b in range(2):
        zown[b : b + 1] = natural(zc, b)
    z_all[0, me] = zown[...].astype(BF16)
    gather(z_all.at[0, me], z_all.at[0], ag_send.at[1], ag_recv.at[1])
    gather(obj_all.at[me], obj_all, obj_send, obj_recv)
    first_dw = contract(z_all.at[0], ag_recv.at[1]) * (2.0 / devices)
    margins_scatter(to_row(first_dw), 2)
    v2 = v1 + scattered(2)
    sweep(v2)
    for b in range(2):
        zown[b : b + 1] = natural(zc, b)
    z_all[1, me] = zown[...].astype(BF16)
    gather(z_all.at[1, me], z_all.at[1], ag_send.at[2], ag_recv.at[2])
    for b in range(2):
        result_ref[1 + b : 2 + b] = sign[b : b + 1] * natural(ac, b)
    for dz in PLANES:
        arrived(obj_all, obj_recv, dz)
    result_ref[3:4] = jnp.sum(obj_all[...], axis=0)
    for phase in range(3):
        drain(send.at[phase], rs_send.at[phase])
    drain(h_all, ag_send.at[0])
    drain(z_all.at[0], ag_send.at[1])
    drain(obj_all, obj_send)
    for b in range(5):
        bulk_wait(b, bulk_send)
    for j in range(4):
        pltpu.make_async_copy(mid.at[j], mid.at[j], mid_send.at[j]).wait()
    pltpu.make_async_copy(fin, fin, fin_send).wait()
    second_dw = contract(z_all.at[1], ag_recv.at[2]) * (2.0 / devices)
    result_ref[0:1, :local] = to_row(primal + first_dw + second_dw)
    drain(z_all.at[1], ag_send.at[2])


def finish(result, weights, alpha, objective):
    weights[...] = result[0:1, : weights.shape[1]]
    alpha[...] = result[1:3]
    objective[...] = result[3:4]


def solution(mesh):
    devices = mesh.shape[AXIS]

    def body(data_t, labels, sample_weight, w_start, alpha_start, visit_order):
        local, samples = data_t.shape
        per = samples // devices
        anyspace = pl.BlockSpec(memory_space=pl.ANY)
        vmem = pl.BlockSpec(memory_space=pltpu.VMEM)
        square = pltpu.VMEM((per, 128), F32)
        dma = pltpu.SemaphoreType.DMA
        result = pl.pallas_call(
            functools.partial(kernel, devices, samples),
            out_shape=jax.ShapeDtypeStruct((4, 128), F32),
            in_specs=[anyspace] * 6,
            out_specs=vmem,
            scratch_shapes=[
                pltpu.VMEM((local, samples), BF16),
                pltpu.VMEM((16, 8, local, per), BF16),
                pltpu.VMEM((16, 272, 128), BF16),
                pltpu.VMEM((4, 3, 272, 128), BF16),
                pltpu.VMEM((4, 272, 128), BF16),
                pltpu.VMEM((3, 272, 128), BF16),
                pltpu.VMEM((272, 128), F32),
                pltpu.VMEM((2, 128), jnp.int32),
                pltpu.VMEM((2, 128), F32),
                pltpu.VMEM((1, local), F32),
                pltpu.VMEM((2, 128), F32),
                pltpu.VMEM((2, 128), jnp.int32),
                pltpu.VMEM((3, devices, 2, 128), F32),
                pltpu.VMEM((3, devices, 2, 128), F32),
                pltpu.VMEM((devices, 2, 128), BF16),
                pltpu.VMEM((2, devices, 2, 128), BF16),
                pltpu.VMEM((devices, 1, 128), F32),
                pltpu.VMEM((per, per), F32),
                pltpu.VMEM((2, 128, 128), F32),
                pltpu.VMEM((2, 128, 128), BF16),
                *[square] * 7,
                pltpu.VMEM((2, 128), F32),
                dma((4,)), dma((5,)), dma((16,)), dma((5,)), dma((5,)), dma((4,)), dma((4,)), dma, dma,
                dma((3,)), dma((3,)), dma((3,)), dma((3, 4)), dma, dma((4,)),
            ],
            compiler_params=pltpu.CompilerParams(
                collective_id=0, has_side_effects=True, vmem_limit_bytes=61998 * 1024
            ),
        )(
            data_t,
            labels.reshape(devices, 2, 128),
            sample_weight.reshape(devices, 2, 128),
            w_start.reshape(1, local),
            alpha_start.reshape(2, 128),
            visit_order,
        )
        weights, alpha, objective = pl.pallas_call(
            finish,
            out_shape=(
                jax.ShapeDtypeStruct((1, local), F32),
                jax.ShapeDtypeStruct((2, 128), F32),
                jax.ShapeDtypeStruct((1, 128), F32),
            ),
            in_specs=[vmem],
            out_specs=(vmem,) * 3,
            compiler_params=pltpu.CompilerParams(vmem_limit_bytes=1024 * 1024),
        )(result)
        return weights.reshape(local), alpha.reshape(per), objective[0, 0]

    return jax.shard_map(
        body,
        mesh=mesh,
        in_specs=(P(AXIS, None), P(), P(), P(AXIS), P(AXIS), P(AXIS, None)),
        out_specs=(P(AXIS), P(AXIS), P()),
        check_vma=False,
    )
```

```python
import functools

import jax
import jax.numpy as jnp
from jax import lax
from jax.experimental import pallas as pl
from jax.experimental.pallas import tpu as pltpu
from jax.sharding import PartitionSpec as P

F32 = jnp.float32
BF16 = jnp.bfloat16
MESH = pl.DeviceIdType.MESH
AXIS = "shard"
GROUP = 16
ORDER = (2, 1, 3, 0)


def kernel(devices, samples, x_hbm, lab_hbm, wgt_hbm, w_hbm, start_hbm, visit_hbm,
           result_ref,
           x, raw, pout, mid, psum, fin, own_sum, own_lab, own_wgt, w_ref, start_ref, visit_ref,
           send, recv, h_all, z_all, obj_all,
           gram, onehot, onehot_t, mc, yc, lc, cc, ac, ic, zc, zown,
           load_sem, small_sem, own_sem, bulk_send, bulk_recv, mid_send, mid_recv, fin_send, fin_recv,
           rs_send, rs_recv, ag_send, ag_recv, obj_send, obj_recv):
    me = lax.axis_index(AXIS)
    local = x.shape[0]
    features = local * devices
    rows = 256
    others = devices - 1

    my_z, my_x, my_y, my_c = me // 32, lax.rem(me // 8, 4), lax.rem(me // 2, 4), lax.rem(me, 2)
    near = [
        lax.rem(my_y + dy, 4) * 2 + lax.rem(my_c + dc, 2)
        for dy in (2, 1, 3, 0)
        for dc in (1, 0)
    ]

    def plane(dz, visit):
        z = lax.rem(my_z + dz, 4)

        def one(dx, carry):
            for place in near:
                visit(z * 32 + lax.rem(my_x + dx, 4) * 8 + place)
            return carry

        if dz:
            lax.fori_loop(2, 6, one, 0)
        else:
            lax.fori_loop(1, 4, one, 0)
            for place in near[:7]:
                visit(z * 32 + my_x * 8 + place)

    PLANES = (2, 1, 3, 0)

    def peers(visit):
        for dz in PLANES:
            plane(dz, visit)

    barrier = pltpu.get_barrier_semaphore()

    def greet(to):
        pl.semaphore_signal(barrier, inc=1, device_id=(to,), device_id_type=MESH)

    pieces = load_sem.shape[0]
    width = samples // pieces

    def load(i):
        at = pl.ds(i * width, width)
        return pltpu.make_async_copy(x_hbm.at[:, at], x.at[:, at], load_sem.at[i])

    small = [
        pltpu.make_async_copy(src, dst, small_sem.at[i])
        for i, (src, dst) in enumerate(
            (
                (w_hbm, w_ref),
                (lab_hbm.at[me], own_lab),
                (wgt_hbm.at[me], own_wgt),
                (start_hbm, start_ref),
                (visit_hbm, visit_ref),
            )
        )
    ]
    small[0].start()
    for i in range(pieces):
        load(i).start()
    peers(greet)
    for copy in small[1:]:
        copy.start()

    def slice_of(to):
        return pl.ds(pl.multiple_of(to * rows, rows), rows)

    def device(z, xx, y, core):
        return ((z * 4 + xx) * 4 + y) * 2 + core

    def line_of(entry):
        return entry % 3 if entry < 12 else (entry - 12) // 2

    def owner_of(entry, place, core):
        line = line_of(entry)
        if entry >= 12:
            y = entry - 12
            other = lax.rem(11 - place - y, 4)
            return device(place, other, y, core) if line == 0 else device(other, place, y, core)
        away = ORDER[entry // 3]
        if line == 2:
            z = lax.rem(my_z + away, 4)
            return device(z, lax.rem(10 - z - place, 4), place, core)
        y = lax.rem(my_y + away, 4)
        other = lax.rem(8 + line - place - y, 4)
        return device(place, other, y, core) if line == 0 else device(other, place, y, core)

    def collector(line, place, core):
        at = [my_z, my_x, my_y]
        at[line] = place
        return device(*at, core)

    my_place = (my_z, my_x, my_y)

    def entries(b):
        return range(12, 16) if b == 4 else range(3 * b, 3 * b + 3)

    def own_slices(b):
        return [
            pltpu.make_async_copy(
                x_hbm.at[:, slice_of(owner_of(e, my_place[line_of(e)], my_c))],
                raw.at[e, my_place[line_of(e)] * 2 + my_c],
                own_sem.at[e],
            )
            for e in entries(b)
        ]

    def bulk(b):
        for step, other in ((1, 0), (3, 0), (2, 1), (0, 1), (1, 1), (3, 1), (2, 0)):
            for e in entries(b):
                line = line_of(e)
                place = lax.rem(my_place[line] + step, 4)
                core = lax.rem(my_c + other, 2)
                pltpu.make_async_remote_copy(
                    src_ref=x.at[:, slice_of(owner_of(e, place, core))],
                    dst_ref=raw.at[e, my_place[line] * 2 + my_c],
                    send_sem=bulk_send.at[b], recv_sem=bulk_recv.at[b],
                    device_id=(collector(line, place, core),), device_id_type=MESH,
                ).start()

    def bulk_wait(b, sem):
        part = entries(b)
        slots = raw.at[pl.ds(part[0], len(part)), pl.ds(0, 7)]
        pltpu.make_async_copy(slots, slots, sem.at[b]).wait()

    lane = lax.broadcasted_iota(jnp.int32, (128, 128), 1)
    sub = lax.broadcasted_iota(jnp.int32, (128, 128), 0)

    def push(entry, j, slot, z, y):
        pltpu.make_async_remote_copy(
            src_ref=pout.at[entry], dst_ref=mid.at[j, slot],
            send_sem=mid_send.at[j], recv_sem=mid_recv.at[j],
            device_id=(device(z, my_x, y, my_c),), device_id_type=MESH,
        ).start()

    def partial_gram(b):
        for copy in own_slices(b):
            copy.wait()
        bulk_wait(b, bulk_recv)
        for e in entries(b):
            piece = raw[e].reshape(8 * local, rows)
            full = lax.dot_general(
                piece, piece, (((0,), (0,)), ((), ())), preferred_element_type=F32
            )
            first, last = full[:128, :128], full[128:, 128:]
            pout[e, 0:128] = jnp.where(sub > lane, first, last).astype(BF16)
            pout[e, 128:256] = full[128:, :128].astype(BF16)
            diag = jnp.sum(jnp.where(sub == lane, first, 0.0), axis=0, keepdims=True)
            pout[e, 256:272] = jnp.broadcast_to(diag, (16, 128)).astype(BF16)
            if e < 9:
                away = ORDER[e // 3]
                if line_of(e) == 2:
                    push(e, 2, e // 3, lax.rem(my_z + away, 4), my_y)
                else:
                    push(e, line_of(e), e // 3, my_z, lax.rem(my_y + away, 4))
        if b == 4:
            for dy in (2, 1, 3):
                y = lax.rem(my_y + dy, 4)
                push(12 + y, 3, dy - 1, my_z, y)

    def middle(j):
        pltpu.make_async_copy(mid.at[j], mid.at[j], mid_recv.at[j]).wait()
        own = pout[9 + j] if j < 3 else pout[12 + my_y]
        total = own.astype(F32) + jnp.sum(mid[j].astype(F32), axis=0)
        along_x = lax.rem(8 + j - my_z - my_y, 4)
        along_z = lax.rem(8 + j - my_x - my_y, 4)
        turn = {0: 0, 1: 1, 2: 0, 3: my_y // 2}[j]
        z = my_z * (1 - turn) + along_z * turn
        xx = along_x * (1 - turn) + my_x * turn
        slot = lax.rem(z - my_z + xx - my_x + 4, 4) - 1
        mine = lax.rem(my_z + my_x + my_y, 4) == j

        @pl.when(mine)
        def _():
            own_sum[...] = total

        @pl.when(jnp.logical_not(mine))
        def _():
            psum[j] = total.astype(BF16)
            pltpu.make_async_remote_copy(
                src_ref=psum.at[j], dst_ref=fin.at[slot],
                send_sem=fin_send, recv_sem=fin_recv,
                device_id=(device(z, xx, my_y, my_c),), device_id_type=MESH,
            ).start()

    for b in (4, 0, 1, 2, 3):
        for copy in own_slices(b):
            copy.start()

    eye = lax.broadcasted_iota(jnp.int32, (local, local), 0) == lax.broadcasted_iota(
        jnp.int32, (local, local), 1
    )

    def to_row(col):
        return jnp.sum(jnp.where(eye, col, 0.0), axis=0, keepdims=True)

    def to_col(row):
        return jnp.sum(jnp.where(eye, row, 0.0), axis=1, keepdims=True)

    chunk = samples // 4

    def margins(row, phase, first, last):
        lhs = jnp.broadcast_to(row, (8, local)).astype(BF16)

        def one(i, carry):
            out = jnp.dot(
                lhs, x[:, pl.ds(pl.multiple_of(i * chunk, chunk), chunk)],
                preferred_element_type=F32,
            )
            for j in range(chunk // 128):
                send[phase, i * (chunk // rows) + j // 2, j % 2 : j % 2 + 1, :] = out[
                    0:1, 128 * j : 128 * j + 128
                ]
            return carry

        lax.fori_loop(first, last, one, 0)

    def scatter(phase, before):
        def one(to):
            pltpu.make_async_remote_copy(
                src_ref=send.at[phase, to], dst_ref=recv.at[phase, me],
                send_sem=rs_send.at[phase], recv_sem=rs_recv.at[phase],
                device_id=(to,), device_id_type=MESH,
            ).start()

        for dz in PLANES:
            before(lax.rem(my_z + dz, 4))
            plane(dz, one)
        recv[phase, me] = send[phase, me]

    def margins_scatter(row, phase):
        scatter(phase, lambda z: margins(row, phase, z, z + 1))

    def scattered(phase):
        many = recv.at[phase, pl.ds(0, others)]
        pltpu.make_async_copy(many, many, rs_recv.at[phase]).wait()
        return jnp.sum(recv[phase], axis=0)

    def gather(src, buf, send_sem, recv_sem):
        for dz in PLANES:

            def one(to):
                pltpu.make_async_remote_copy(
                    src_ref=src, dst_ref=buf.at[me],
                    send_sem=send_sem, recv_sem=recv_sem.at[dz],
                    device_id=(to,), device_id_type=MESH,
                ).start()

            plane(dz, one)

    def arrived(buf, sem, dz):
        many = buf.at[pl.ds(0, devices // 4 - (dz == 0))]
        pltpu.make_async_copy(many, many, sem.at[dz]).wait()

    def drain(buf, sem):
        many = buf.at[pl.ds(0, others)]
        pltpu.make_async_copy(many, many, sem).wait()

    def contract(buf, sem):
        acc = jnp.zeros((local, 128), F32)
        for dz in PLANES[::-1]:
            arrived(buf, sem, dz)
            first = lax.rem(my_z + 4 - dz, 4) * 32

            def one(i, acc):
                d = first + i
                part = x[:, pl.ds(pl.multiple_of(d * rows, rows), rows)].astype(F32)
                v = buf[d].astype(F32)
                return acc + part[:, :128] * v[0:1] + part[:, 128:] * v[1:2]

            acc = lax.fori_loop(0, 32, one, acc, unroll=4)
        return jnp.sum(acc, axis=1, keepdims=True)

    small[0].wait()
    w_row = w_ref[...]
    per = width // chunk
    for i in range(pieces):
        load(i).wait()
        margins(w_row, 0, i * per, (i + 1) * per)
    pl.semaphore_wait(barrier, others)
    scatter(0, lambda z: None)
    bulk(4)
    bulk(0)
    bulk(1)

    def square(d, acc):
        part = x[:, pl.ds(pl.multiple_of(d * rows, rows), rows)].astype(F32)
        return acc + part[:, :128] * part[:, :128] + part[:, 128:] * part[:, 128:]

    sq = lax.fori_loop(0, devices, square, jnp.zeros((local, 128), F32), unroll=4)
    scale = jnp.sum(sq, axis=1, keepdims=True) / samples + 1e-06
    for copy in small[1:]:
        copy.wait()
    sign = own_lab[...].astype(F32)
    bound = own_wgt[...]

    v0 = scattered(0)
    h_all[me] = (bound * sign * jnp.maximum(0.0, 1.0 - sign * v0)).astype(BF16)
    gather(h_all.at[me], h_all, ag_send.at[0], ag_recv.at[0])
    bulk(2)
    bulk(3)
    alpha0 = bound * start_ref[...]

    def permuted(vec, b):
        col = jnp.sum(onehot[b] * vec[b : b + 1], axis=1, keepdims=True)
        return jnp.broadcast_to(col, (128, 128))

    for b in range(2):
        hot = jnp.where(sub == visit_ref[b : b + 1, :], 1.0, 0.0)
        onehot_t[b] = hot.astype(BF16)
        onehot[b] = jnp.transpose(hot)
    for b in range(2):
        part = slice(128 * b, 128 * b + 128)
        yc[part] = permuted(sign, b)
        edge = yc[part] * permuted(bound, b)
        lc[part] = jnp.minimum(edge, 0.0)
        cc[part] = jnp.maximum(edge, 0.0)
        ac[part] = yc[part] * permuted(alpha0, b)

    partial_gram(4)
    partial_gram(0)
    partial_gram(1)
    partial_gram(2)
    w_col = to_col(w_row)
    stepped = w_col + contract(h_all, ag_recv.at[0]) / (samples * scale)
    thresh = 1.0 / (4.0 * features * scale)
    primal = stepped - jnp.clip(stepped, -thresh, thresh)
    penalty = jnp.sum(jnp.abs(primal)) / (4.0 * features)
    margins_scatter(to_row(primal), 1)
    partial_gram(3)
    middle(3)
    middle(2)
    middle(1)
    middle(0)
    v1 = scattered(1)
    loss = jnp.sum(bound * jnp.square(jnp.maximum(0.0, 1.0 - sign * v1))) / (2.0 * samples)
    obj_all[me] = jnp.full((1, 128), loss + penalty, F32)

    pltpu.make_async_copy(fin, fin, fin_recv).wait()

    def halves(a):
        hi = a.astype(BF16)
        return hi, (a - hi.astype(F32)).astype(BF16)

    def reordered(a, b1, b2):
        hi, lo = halves(a)
        mid = jnp.dot(hi, onehot_t[b2], preferred_element_type=F32) + jnp.dot(
            lo, onehot_t[b2], preferred_element_type=F32
        )
        hi, lo = halves(mid)
        left = onehot[b1].astype(BF16)
        return jnp.dot(left, hi, preferred_element_type=F32) + jnp.dot(
            left, lo, preferred_element_type=F32
        )

    def whole(first, last):
        return own_sum[first:last] + jnp.sum(fin[:, first:last].astype(F32), axis=0)

    packed = whole(0, 128)
    turned = jnp.transpose(packed)
    diag_row = whole(256, 272)[0:1]
    first_block = jnp.where(sub > lane, packed, jnp.where(sub < lane, turned, diag_row))
    last_block = jnp.where(sub > lane, turned, packed)
    gram[0:128, 0:128] = reordered(first_block, 0, 0)
    gram[128:256, 0:128] = reordered(whole(128, 256), 1, 0)
    gram[128:256, 128:256] = reordered(last_block, 1, 1)
    for b in range(2):
        part = slice(128 * b, 128 * b + 128)
        diag = jnp.sum(jnp.where(lane == sub, gram[part, part], 0.0), axis=1, keepdims=True)
        ic[part] = jnp.broadcast_to(1.0 / (2.0 * (diag + 1e-06)), (128, 128))

    lane16 = lax.broadcasted_iota(jnp.int32, (GROUP, 128), 1)
    sub16 = lax.broadcasted_iota(jnp.int32, (GROUP, 128), 0)

    def sweep(margin):
        for b in range(2):
            part = slice(128 * b, 128 * b + 128)
            mc[part] = ac[part] + (yc[part] - permuted(margin, b)) * ic[part]
        c = [jnp.zeros((1, 128), F32), jnp.zeros((1, 128), F32)]
        for t in range(rows // GROUP):
            at = slice(GROUP * t, GROUP * t + GROUP)
            b, first = t // 8, GROUP * (t % 8)
            aim = mc[at]
            if t:
                prod = gram[at, 0:128] * c[0]
                if b:
                    prod = prod + gram[at, 128:256] * c[1]
                aim = aim - 2.0 * ic[at] * jnp.sum(prod, axis=1, keepdims=True)
            new = jnp.minimum(jnp.maximum(aim, lc[at]), cc[at])
            step = new - ac[at]
            ac[at] = new
            zc[at] = step
            c[b] = c[b] + jnp.sum(
                jnp.where(lane16 == sub16 + first, step, 0.0), axis=0, keepdims=True
            )

    def natural(col, b):
        return jnp.sum(onehot[b] * col[128 * b : 128 * b + 128], axis=0, keepdims=True)

    sweep(v1)
    for b in range(2):
        zown[b : b + 1] = natural(zc, b)
    z_all[0, me] = zown[...].astype(BF16)
    gather(z_all.at[0, me], z_all.at[0], ag_send.at[1], ag_recv.at[1])
    gather(obj_all.at[me], obj_all, obj_send, obj_recv)
    first_dw = contract(z_all.at[0], ag_recv.at[1]) * (2.0 / devices)
    margins_scatter(to_row(first_dw), 2)
    v2 = v1 + scattered(2)
    sweep(v2)
    for b in range(2):
        zown[b : b + 1] = natural(zc, b)
    z_all[1, me] = zown[...].astype(BF16)
    gather(z_all.at[1, me], z_all.at[1], ag_send.at[2], ag_recv.at[2])
    for b in range(2):
        result_ref[1 + b : 2 + b] = sign[b : b + 1] * natural(ac, b)
    for dz in PLANES:
        arrived(obj_all, obj_recv, dz)
    result_ref[3:4] = jnp.sum(obj_all[...], axis=0)
    for phase in range(3):
        drain(send.at[phase], rs_send.at[phase])
    drain(h_all, ag_send.at[0])
    drain(z_all.at[0], ag_send.at[1])
    drain(obj_all, obj_send)
    for b in range(5):
        bulk_wait(b, bulk_send)
    for j in range(4):
        pltpu.make_async_copy(mid.at[j], mid.at[j], mid_send.at[j]).wait()
    pltpu.make_async_copy(fin, fin, fin_send).wait()
    second_dw = contract(z_all.at[1], ag_recv.at[2]) * (2.0 / devices)
    result_ref[0:1, :local] = to_row(primal + first_dw + second_dw)
    drain(z_all.at[1], ag_send.at[2])


def finish(result, weights, alpha, objective):
    weights[...] = result[0:1, : weights.shape[1]]
    alpha[...] = result[1:3]
    objective[...] = result[3:4]


def solution(mesh):
    devices = mesh.shape[AXIS]

    def body(data_t, labels, sample_weight, w_start, alpha_start, visit_order):
        local, samples = data_t.shape
        per = samples // devices
        anyspace = pl.BlockSpec(memory_space=pl.ANY)
        vmem = pl.BlockSpec(memory_space=pltpu.VMEM)
        square = pltpu.VMEM((per, 128), F32)
        dma = pltpu.SemaphoreType.DMA
        result = pl.pallas_call(
            functools.partial(kernel, devices, samples),
            out_shape=jax.ShapeDtypeStruct((4, 128), F32),
            in_specs=[anyspace] * 6,
            out_specs=vmem,
            scratch_shapes=[
                pltpu.VMEM((local, samples), BF16),
                pltpu.VMEM((16, 8, local, per), BF16),
                pltpu.VMEM((16, 272, 128), BF16),
                pltpu.VMEM((4, 3, 272, 128), BF16),
                pltpu.VMEM((4, 272, 128), BF16),
                pltpu.VMEM((3, 272, 128), BF16),
                pltpu.VMEM((272, 128), F32),
                pltpu.VMEM((2, 128), jnp.int32),
                pltpu.VMEM((2, 128), F32),
                pltpu.VMEM((1, local), F32),
                pltpu.VMEM((2, 128), F32),
                pltpu.VMEM((2, 128), jnp.int32),
                pltpu.VMEM((3, devices, 2, 128), F32),
                pltpu.VMEM((3, devices, 2, 128), F32),
                pltpu.VMEM((devices, 2, 128), BF16),
                pltpu.VMEM((2, devices, 2, 128), BF16),
                pltpu.VMEM((devices, 1, 128), F32),
                pltpu.VMEM((per, per), F32),
                pltpu.VMEM((2, 128, 128), F32),
                pltpu.VMEM((2, 128, 128), BF16),
                *[square] * 7,
                pltpu.VMEM((2, 128), F32),
                dma((4,)), dma((5,)), dma((16,)), dma((5,)), dma((5,)), dma((4,)), dma((4,)), dma, dma,
                dma((3,)), dma((3,)), dma((3,)), dma((3, 4)), dma, dma((4,)),
            ],
            compiler_params=pltpu.CompilerParams(
                collective_id=0, has_side_effects=True, vmem_limit_bytes=61998 * 1024
            ),
        )(
            data_t,
            labels.reshape(devices, 2, 128),
            sample_weight.reshape(devices, 2, 128),
            w_start.reshape(1, local),
            alpha_start.reshape(2, 128),
            visit_order,
        )
        weights, alpha, objective = pl.pallas_call(
            finish,
            out_shape=(
                jax.ShapeDtypeStruct((1, local), F32),
                jax.ShapeDtypeStruct((2, 128), F32),
                jax.ShapeDtypeStruct((1, 128), F32),
            ),
            in_specs=[vmem],
            out_specs=(vmem,) * 3,
            compiler_params=pltpu.CompilerParams(vmem_limit_bytes=1024 * 1024),
        )(result)
        return weights.reshape(local), alpha.reshape(per), objective[0, 0]

    return jax.shard_map(
        body,
        mesh=mesh,
        in_specs=(P(AXIS, None), P(), P(), P(AXIS), P(AXIS), P(AXIS, None)),
        out_specs=(P(AXIS), P(AXIS), P()),
        check_vma=False,
    )
```

```python
import functools

import jax
import jax.numpy as jnp
from jax import lax
from jax.experimental import pallas as pl
from jax.experimental.pallas import tpu as pltpu
from jax.sharding import PartitionSpec as P

F32 = jnp.float32
BF16 = jnp.bfloat16
MESH = pl.DeviceIdType.MESH
AXIS = "shard"
GROUP = 16
ORDER = (2, 1, 3, 0)


def kernel(devices, samples, x_hbm, lab_hbm, wgt_hbm, w_hbm, start_hbm, visit_hbm,
           result_ref,
           x, raw, pout, mid, psum, fin, own_sum, own_lab, own_wgt, w_ref, start_ref, visit_ref,
           send, recv, h_all, z_all, obj_all,
           gram, onehot, onehot_t, mc, yc, lc, cc, ac, ic, zc, zown,
           load_sem, small_sem, own_sem, bulk_send, bulk_recv, mid_send, mid_recv, fin_send, fin_recv,
           rs_send, rs_recv, ag_send, ag_recv, obj_send, obj_recv):
    me = lax.axis_index(AXIS)
    local = x.shape[0]
    features = local * devices
    rows = 256
    others = devices - 1

    my_z, my_x, my_y, my_c = me // 32, lax.rem(me // 8, 4), lax.rem(me // 2, 4), lax.rem(me, 2)
    near = [
        lax.rem(my_y + dy, 4) * 2 + lax.rem(my_c + dc, 2)
        for dy in (2, 1, 3, 0)
        for dc in (1, 0)
    ]

    def plane(dz, visit):
        z = lax.rem(my_z + dz, 4)

        def one(dx, carry):
            for place in near:
                visit(z * 32 + lax.rem(my_x + dx, 4) * 8 + place)
            return carry

        if dz:
            lax.fori_loop(2, 6, one, 0)
        else:
            lax.fori_loop(1, 4, one, 0)
            for place in near[:7]:
                visit(z * 32 + my_x * 8 + place)

    PLANES = (2, 1, 3, 0)

    def peers(visit):
        for dz in PLANES:
            plane(dz, visit)

    barrier = pltpu.get_barrier_semaphore()

    def greet(to):
        pl.semaphore_signal(barrier, inc=1, device_id=(to,), device_id_type=MESH)

    pieces = load_sem.shape[0]
    width = samples // pieces

    def load(i):
        at = pl.ds(i * width, width)
        return pltpu.make_async_copy(x_hbm.at[:, at], x.at[:, at], load_sem.at[i])

    small = [
        pltpu.make_async_copy(src, dst, small_sem.at[i])
        for i, (src, dst) in enumerate(
            (
                (w_hbm, w_ref),
                (lab_hbm.at[me], own_lab),
                (wgt_hbm.at[me], own_wgt),
                (start_hbm, start_ref),
                (visit_hbm, visit_ref),
            )
        )
    ]
    small[0].start()
    for i in range(pieces):
        load(i).start()
    peers(greet)
    for copy in small[1:]:
        copy.start()

    def slice_of(to):
        return pl.ds(pl.multiple_of(to * rows, rows), rows)

    def device(z, xx, y, core):
        return ((z * 4 + xx) * 4 + y) * 2 + core

    def line_of(entry):
        return entry % 3 if entry < 12 else (entry - 12) // 2

    def owner_of(entry, place, core):
        line = line_of(entry)
        if entry >= 12:
            y = entry - 12
            other = lax.rem(11 - place - y, 4)
            return device(place, other, y, core) if line == 0 else device(other, place, y, core)
        away = ORDER[entry // 3]
        if line == 2:
            xx = lax.rem(my_x + away, 4)
            return device(lax.rem(10 - xx - place, 4), xx, place, core)
        y = lax.rem(my_y + away, 4)
        other = lax.rem(8 + line - place - y, 4)
        return device(place, other, y, core) if line == 0 else device(other, place, y, core)

    def collector(line, place, core):
        at = [my_z, my_x, my_y]
        at[line] = place
        return device(*at, core)

    my_place = (my_z, my_x, my_y)

    def entries(b):
        return range(12, 16) if b == 4 else range(3 * b, 3 * b + 3)

    def own_slices(b):
        return [
            pltpu.make_async_copy(
                x_hbm.at[:, slice_of(owner_of(e, my_place[line_of(e)], my_c))],
                raw.at[e, my_place[line_of(e)] * 2 + my_c],
                own_sem.at[e],
            )
            for e in entries(b)
        ]

    def bulk(b):
        for step, other in ((1, 0), (3, 0), (2, 1), (0, 1), (1, 1), (3, 1), (2, 0)):
            for e in entries(b):
                line = line_of(e)
                place = lax.rem(my_place[line] + step, 4)
                core = lax.rem(my_c + other, 2)
                pltpu.make_async_remote_copy(
                    src_ref=x.at[:, slice_of(owner_of(e, place, core))],
                    dst_ref=raw.at[e, my_place[line] * 2 + my_c],
                    send_sem=bulk_send.at[b], recv_sem=bulk_recv.at[b],
                    device_id=(collector(line, place, core),), device_id_type=MESH,
                ).start()

    def bulk_wait(b, sem):
        part = entries(b)
        slots = raw.at[pl.ds(part[0], len(part)), pl.ds(0, 7)]
        pltpu.make_async_copy(slots, slots, sem.at[b]).wait()

    lane = lax.broadcasted_iota(jnp.int32, (128, 128), 1)
    sub = lax.broadcasted_iota(jnp.int32, (128, 128), 0)

    def push(entry, j, slot, xx, y):
        pltpu.make_async_remote_copy(
            src_ref=pout.at[entry], dst_ref=mid.at[j, slot],
            send_sem=mid_send.at[j], recv_sem=mid_recv.at[j],
            device_id=(device(my_z, xx, y, my_c),), device_id_type=MESH,
        ).start()

    def partial_gram(b):
        for copy in own_slices(b):
            copy.wait()
        bulk_wait(b, bulk_recv)
        for e in entries(b):
            piece = raw[e].reshape(8 * local, rows)
            full = lax.dot_general(
                piece, piece, (((0,), (0,)), ((), ())), preferred_element_type=F32
            )
            first, last = full[:128, :128], full[128:, 128:]
            pout[e, 0:128] = jnp.where(sub > lane, first, last).astype(BF16)
            pout[e, 128:256] = full[128:, :128].astype(BF16)
            diag = jnp.sum(jnp.where(sub == lane, first, 0.0), axis=0, keepdims=True)
            pout[e, 256:272] = jnp.broadcast_to(diag, (16, 128)).astype(BF16)
            if e < 9:
                away = ORDER[e // 3]
                if line_of(e) == 2:
                    push(e, 2, e // 3, lax.rem(my_x + away, 4), my_y)
                else:
                    push(e, line_of(e), e // 3, my_x, lax.rem(my_y + away, 4))
        if b == 4:
            for dy in (2, 1, 3):
                y = lax.rem(my_y + dy, 4)
                push(12 + y, 3, dy - 1, my_x, y)

    def middle(j):
        pltpu.make_async_copy(mid.at[j], mid.at[j], mid_recv.at[j]).wait()
        own = pout[9 + j] if j < 3 else pout[12 + my_y]
        total = own.astype(F32) + jnp.sum(mid[j].astype(F32), axis=0)
        along_x = lax.rem(8 + j - my_z - my_y, 4)
        along_z = lax.rem(8 + j - my_x - my_y, 4)
        turn = {0: 0, 1: 1, 2: 1, 3: my_y // 2}[j]
        z = my_z * (1 - turn) + along_z * turn
        xx = along_x * (1 - turn) + my_x * turn
        slot = lax.rem(z - my_z + xx - my_x + 4, 4) - 1
        mine = lax.rem(my_z + my_x + my_y, 4) == j

        @pl.when(mine)
        def _():
            own_sum[...] = total

        @pl.when(jnp.logical_not(mine))
        def _():
            psum[j] = total.astype(BF16)
            pltpu.make_async_remote_copy(
                src_ref=psum.at[j], dst_ref=fin.at[slot],
                send_sem=fin_send, recv_sem=fin_recv,
                device_id=(device(z, xx, my_y, my_c),), device_id_type=MESH,
            ).start()

    for b in (4, 0, 1, 2, 3):
        for copy in own_slices(b):
            copy.start()

    eye = lax.broadcasted_iota(jnp.int32, (local, local), 0) == lax.broadcasted_iota(
        jnp.int32, (local, local), 1
    )

    def to_row(col):
        return jnp.sum(jnp.where(eye, col, 0.0), axis=0, keepdims=True)

    def to_col(row):
        return jnp.sum(jnp.where(eye, row, 0.0), axis=1, keepdims=True)

    chunk = samples // 4

    def margins(row, phase, first, last):
        lhs = jnp.broadcast_to(row, (8, local)).astype(BF16)

        def one(i, carry):
            out = jnp.dot(
                lhs, x[:, pl.ds(pl.multiple_of(i * chunk, chunk), chunk)],
                preferred_element_type=F32,
            )
            for j in range(chunk // 128):
                send[phase, i * (chunk // rows) + j // 2, j % 2 : j % 2 + 1, :] = out[
                    0:1, 128 * j : 128 * j + 128
                ]
            return carry

        lax.fori_loop(first, last, one, 0)

    def scatter(phase, before):
        def one(to):
            pltpu.make_async_remote_copy(
                src_ref=send.at[phase, to], dst_ref=recv.at[phase, me],
                send_sem=rs_send.at[phase], recv_sem=rs_recv.at[phase],
                device_id=(to,), device_id_type=MESH,
            ).start()

        for dz in PLANES:
            before(lax.rem(my_z + dz, 4))
            plane(dz, one)
        recv[phase, me] = send[phase, me]

    def margins_scatter(row, phase):
        scatter(phase, lambda z: margins(row, phase, z, z + 1))

    def scattered(phase):
        many = recv.at[phase, pl.ds(0, others)]
        pltpu.make_async_copy(many, many, rs_recv.at[phase]).wait()
        return jnp.sum(recv[phase], axis=0)

    def gather(src, buf, send_sem, recv_sem):
        for dz in PLANES:

            def one(to):
                pltpu.make_async_remote_copy(
                    src_ref=src, dst_ref=buf.at[me],
                    send_sem=send_sem, recv_sem=recv_sem.at[dz],
                    device_id=(to,), device_id_type=MESH,
                ).start()

            plane(dz, one)

    def arrived(buf, sem, dz):
        many = buf.at[pl.ds(0, devices // 4 - (dz == 0))]
        pltpu.make_async_copy(many, many, sem.at[dz]).wait()

    def drain(buf, sem):
        many = buf.at[pl.ds(0, others)]
        pltpu.make_async_copy(many, many, sem).wait()

    def contract(buf, sem):
        acc = jnp.zeros((local, 128), F32)
        for dz in PLANES[::-1]:
            arrived(buf, sem, dz)
            first = lax.rem(my_z + 4 - dz, 4) * 32

            def one(i, acc):
                d = first + i
                part = x[:, pl.ds(pl.multiple_of(d * rows, rows), rows)].astype(F32)
                v = buf[d].astype(F32)
                return acc + part[:, :128] * v[0:1] + part[:, 128:] * v[1:2]

            acc = lax.fori_loop(0, 32, one, acc, unroll=4)
        return jnp.sum(acc, axis=1, keepdims=True)

    small[0].wait()
    w_row = w_ref[...]
    per = width // chunk
    for i in range(pieces):
        load(i).wait()
        margins(w_row, 0, i * per, (i + 1) * per)
    pl.semaphore_wait(barrier, others)
    scatter(0, lambda z: None)
    bulk(4)
    bulk(0)
    bulk(1)

    def square(d, acc):
        part = x[:, pl.ds(pl.multiple_of(d * rows, rows), rows)].astype(F32)
        return acc + part[:, :128] * part[:, :128] + part[:, 128:] * part[:, 128:]

    sq = lax.fori_loop(0, devices, square, jnp.zeros((local, 128), F32), unroll=4)
    scale = jnp.sum(sq, axis=1, keepdims=True) / samples + 1e-06
    for copy in small[1:]:
        copy.wait()
    sign = own_lab[...].astype(F32)
    bound = own_wgt[...]

    v0 = scattered(0)
    h_all[me] = (bound * sign * jnp.maximum(0.0, 1.0 - sign * v0)).astype(BF16)
    gather(h_all.at[me], h_all, ag_send.at[0], ag_recv.at[0])
    bulk(2)
    bulk(3)
    alpha0 = bound * start_ref[...]

    def permuted(vec, b):
        col = jnp.sum(onehot[b] * vec[b : b + 1], axis=1, keepdims=True)
        return jnp.broadcast_to(col, (128, 128))

    for b in range(2):
        hot = jnp.where(sub == visit_ref[b : b + 1, :], 1.0, 0.0)
        onehot_t[b] = hot.astype(BF16)
        onehot[b] = jnp.transpose(hot)
    for b in range(2):
        part = slice(128 * b, 128 * b + 128)
        yc[part] = permuted(sign, b)
        edge = yc[part] * permuted(bound, b)
        lc[part] = jnp.minimum(edge, 0.0)
        cc[part] = jnp.maximum(edge, 0.0)
        ac[part] = yc[part] * permuted(alpha0, b)

    partial_gram(4)
    partial_gram(0)
    partial_gram(1)
    partial_gram(2)
    w_col = to_col(w_row)
    stepped = w_col + contract(h_all, ag_recv.at[0]) / (samples * scale)
    thresh = 1.0 / (4.0 * features * scale)
    primal = stepped - jnp.clip(stepped, -thresh, thresh)
    penalty = jnp.sum(jnp.abs(primal)) / (4.0 * features)
    margins_scatter(to_row(primal), 1)
    partial_gram(3)
    middle(3)
    middle(2)
    middle(1)
    middle(0)
    v1 = scattered(1)
    loss = jnp.sum(bound * jnp.square(jnp.maximum(0.0, 1.0 - sign * v1))) / (2.0 * samples)
    obj_all[me] = jnp.full((1, 128), loss + penalty, F32)

    pltpu.make_async_copy(fin, fin, fin_recv).wait()

    def halves(a):
        hi = a.astype(BF16)
        return hi, (a - hi.astype(F32)).astype(BF16)

    def reordered(a, b1, b2):
        hi, lo = halves(a)
        mid = jnp.dot(hi, onehot_t[b2], preferred_element_type=F32) + jnp.dot(
            lo, onehot_t[b2], preferred_element_type=F32
        )
        hi, lo = halves(mid)
        left = onehot[b1].astype(BF16)
        return jnp.dot(left, hi, preferred_element_type=F32) + jnp.dot(
            left, lo, preferred_element_type=F32
        )

    def whole(first, last):
        return own_sum[first:last] + jnp.sum(fin[:, first:last].astype(F32), axis=0)

    packed = whole(0, 128)
    turned = jnp.transpose(packed)
    diag_row = whole(256, 272)[0:1]
    first_block = jnp.where(sub > lane, packed, jnp.where(sub < lane, turned, diag_row))
    last_block = jnp.where(sub > lane, turned, packed)
    gram[0:128, 0:128] = reordered(first_block, 0, 0)
    gram[128:256, 0:128] = reordered(whole(128, 256), 1, 0)
    gram[128:256, 128:256] = reordered(last_block, 1, 1)
    for b in range(2):
        part = slice(128 * b, 128 * b + 128)
        diag = jnp.sum(jnp.where(lane == sub, gram[part, part], 0.0), axis=1, keepdims=True)
        ic[part] = jnp.broadcast_to(1.0 / (2.0 * (diag + 1e-06)), (128, 128))

    lane16 = lax.broadcasted_iota(jnp.int32, (GROUP, 128), 1)
    sub16 = lax.broadcasted_iota(jnp.int32, (GROUP, 128), 0)

    def sweep(margin):
        for b in range(2):
            part = slice(128 * b, 128 * b + 128)
            mc[part] = ac[part] + (yc[part] - permuted(margin, b)) * ic[part]
        c = [jnp.zeros((1, 128), F32), jnp.zeros((1, 128), F32)]
        for t in range(rows // GROUP):
            at = slice(GROUP * t, GROUP * t + GROUP)
            b, first = t // 8, GROUP * (t % 8)
            aim = mc[at]
            if t:
                prod = gram[at, 0:128] * c[0]
                if b:
                    prod = prod + gram[at, 128:256] * c[1]
                aim = aim - 2.0 * ic[at] * jnp.sum(prod, axis=1, keepdims=True)
            new = jnp.minimum(jnp.maximum(aim, lc[at]), cc[at])
            step = new - ac[at]
            ac[at] = new
            zc[at] = step
            c[b] = c[b] + jnp.sum(
                jnp.where(lane16 == sub16 + first, step, 0.0), axis=0, keepdims=True
            )

    def natural(col, b):
        return jnp.sum(onehot[b] * col[128 * b : 128 * b + 128], axis=0, keepdims=True)

    sweep(v1)
    for b in range(2):
        zown[b : b + 1] = natural(zc, b)
    z_all[0, me] = zown[...].astype(BF16)
    gather(z_all.at[0, me], z_all.at[0], ag_send.at[1], ag_recv.at[1])
    gather(obj_all.at[me], obj_all, obj_send, obj_recv)
    first_dw = contract(z_all.at[0], ag_recv.at[1]) * (2.0 / devices)
    margins_scatter(to_row(first_dw), 2)
    v2 = v1 + scattered(2)
    sweep(v2)
    for b in range(2):
        zown[b : b + 1] = natural(zc, b)
    z_all[1, me] = zown[...].astype(BF16)
    gather(z_all.at[1, me], z_all.at[1], ag_send.at[2], ag_recv.at[2])
    for b in range(2):
        result_ref[1 + b : 2 + b] = sign[b : b + 1] * natural(ac, b)
    for dz in PLANES:
        arrived(obj_all, obj_recv, dz)
    result_ref[3:4] = jnp.sum(obj_all[...], axis=0)
    for phase in range(3):
        drain(send.at[phase], rs_send.at[phase])
    drain(h_all, ag_send.at[0])
    drain(z_all.at[0], ag_send.at[1])
    drain(obj_all, obj_send)
    for b in range(5):
        bulk_wait(b, bulk_send)
    for j in range(4):
        pltpu.make_async_copy(mid.at[j], mid.at[j], mid_send.at[j]).wait()
    pltpu.make_async_copy(fin, fin, fin_send).wait()
    second_dw = contract(z_all.at[1], ag_recv.at[2]) * (2.0 / devices)
    result_ref[0:1, :local] = to_row(primal + first_dw + second_dw)
    drain(z_all.at[1], ag_send.at[2])


def finish(result, weights, alpha, objective):
    weights[...] = result[0:1, : weights.shape[1]]
    alpha[...] = result[1:3]
    objective[...] = result[3:4]


def solution(mesh):
    devices = mesh.shape[AXIS]

    def body(data_t, labels, sample_weight, w_start, alpha_start, visit_order):
        local, samples = data_t.shape
        per = samples // devices
        anyspace = pl.BlockSpec(memory_space=pl.ANY)
        vmem = pl.BlockSpec(memory_space=pltpu.VMEM)
        square = pltpu.VMEM((per, 128), F32)
        dma = pltpu.SemaphoreType.DMA
        result = pl.pallas_call(
            functools.partial(kernel, devices, samples),
            out_shape=jax.ShapeDtypeStruct((4, 128), F32),
            in_specs=[anyspace] * 6,
            out_specs=vmem,
            scratch_shapes=[
                pltpu.VMEM((local, samples), BF16),
                pltpu.VMEM((16, 8, local, per), BF16),
                pltpu.VMEM((16, 272, 128), BF16),
                pltpu.VMEM((4, 3, 272, 128), BF16),
                pltpu.VMEM((4, 272, 128), BF16),
                pltpu.VMEM((3, 272, 128), BF16),
                pltpu.VMEM((272, 128), F32),
                pltpu.VMEM((2, 128), jnp.int32),
                pltpu.VMEM((2, 128), F32),
                pltpu.VMEM((1, local), F32),
                pltpu.VMEM((2, 128), F32),
                pltpu.VMEM((2, 128), jnp.int32),
                pltpu.VMEM((3, devices, 2, 128), F32),
                pltpu.VMEM((3, devices, 2, 128), F32),
                pltpu.VMEM((devices, 2, 128), BF16),
                pltpu.VMEM((2, devices, 2, 128), BF16),
                pltpu.VMEM((devices, 1, 128), F32),
                pltpu.VMEM((per, per), F32),
                pltpu.VMEM((2, 128, 128), F32),
                pltpu.VMEM((2, 128, 128), BF16),
                *[square] * 7,
                pltpu.VMEM((2, 128), F32),
                dma((4,)), dma((5,)), dma((16,)), dma((5,)), dma((5,)), dma((4,)), dma((4,)), dma, dma,
                dma((3,)), dma((3,)), dma((3,)), dma((3, 4)), dma, dma((4,)),
            ],
            compiler_params=pltpu.CompilerParams(
                collective_id=0, has_side_effects=True, vmem_limit_bytes=61998 * 1024
            ),
        )(
            data_t,
            labels.reshape(devices, 2, 128),
            sample_weight.reshape(devices, 2, 128),
            w_start.reshape(1, local),
            alpha_start.reshape(2, 128),
            visit_order,
        )
        weights, alpha, objective = pl.pallas_call(
            finish,
            out_shape=(
                jax.ShapeDtypeStruct((1, local), F32),
                jax.ShapeDtypeStruct((2, 128), F32),
                jax.ShapeDtypeStruct((1, 128), F32),
            ),
            in_specs=[vmem],
            out_specs=(vmem,) * 3,
            compiler_params=pltpu.CompilerParams(vmem_limit_bytes=1024 * 1024),
        )(result)
        return weights.reshape(local), alpha.reshape(per), objective[0, 0]

    return jax.shard_map(
        body,
        mesh=mesh,
        in_specs=(P(AXIS, None), P(), P(), P(AXIS), P(AXIS), P(AXIS, None)),
        out_specs=(P(AXIS), P(AXIS), P()),
        check_vma=False,
    )
```
